32 devices in a mesh: curve: 8 (over z, x), head: 4 (over y, core).
Axes of the slice: x: 2, y: 2, z: 4, core: 2. Of those that a mesh axis runs over, the one named last changes fastest.
Arguments:
- points: bfloat16 [16384, 1024], P(('curve', 'head')), may hold values from -6 to 6
- order: int32 [32, 512], P(('curve', 'head')), may hold values from 0 to 511, each once within a row
- scan_ids: int32 [16384], P(('curve', 'head')), may hold values from 0 to 3
- ln_gain: float32 [2, 1024], replicated, may hold values from 0.25 to 1.75
- w_qkv: bfloat16 [2, 1024, 3072], P(None, None, 'head'), may hold values from -7 to 7, as said below
- w_out: bfloat16 [2, 1024, 1024], P(None, 'head'), may hold values from -0.1875 to 0.1875
Outputs:
- refined: bfloat16 [16384, 1024], P(('curve', 'head'))
The draws below stay inside these ranges and needn't reach their ends.
Inputs may be any that keep to these rules, and one draw needn't show every extreme that they name: `order`: row b is a permutation of the 512 rows of block b. `w_qkv`: columns ordered by head, then query, key, value, then entry.
All inputs are finite; a program needn't handle non-finite values.
Results may differ from the reference program's by a relative error of at most 0.01.
Values may be sent and summed in bfloat16 or wider, within the bound.
A program may use at most 64 MiB of HBM per device.

```python
import jax
import jax.numpy as jnp
from jax import lax

D = 1024
HEADS = 16
HEAD_DIM = 64
PATCH = 1024
SCANS = 4
TOK_DEV = 512
TOKENS = 16384
DEVICES = 32


def draw_w_qkv(key, part):
    base = jnp.clip(jax.random.normal(key, (2, D, HEADS, 3, HEAD_DIM), jnp.float32), -5.0, 5.0) * D ** (-0.5)
    return base.reshape(2, D, HEADS * 3 * HEAD_DIM).astype(jnp.bfloat16)


def touch_ends(values, own_key, smallest, largest):
    longest = values.shape.index(max(values.shape))
    spots = []
    for shift in (0, 1):
        where = [jax.random.randint(jax.random.fold_in(own_key, axis), (), 0, length) for axis, length in enumerate(values.shape)]
        where[longest] = (where[longest] + shift) % values.shape[longest]
        spots.append(tuple(where))
    return values.at[spots[0]].set(smallest).at[spots[1]].set(largest)


def level_of(own_key, extent, pieces, smallest, largest):
    def one(axis_at, blocks):
        heights = jax.random.uniform(jax.random.fold_in(jax.random.fold_in(own_key, 6), axis_at), (blocks,), jnp.float32, smallest / len(pieces), largest / len(pieces))
        return jnp.repeat(jnp.exp(heights), extent[axis_at] // blocks).reshape((-1,) + (1,) * (len(extent) - axis_at - 1))

    factor_of = one(*pieces[0])
    for cut in pieces[1:]:
        factor_of = factor_of * one(*cut)
    return factor_of


def normal_values(rng, extent, scale, most, split=(), held_as=jnp.bfloat16):
    level = level_of(rng, extent, split, -0.22, 0.18) if split else 1.0
    result = jax.random.normal(rng, extent, jnp.float32) * scale * level
    return jnp.minimum(jnp.maximum(result, -most), most).astype(held_as)


def setup_inputs(seed: int = 0) -> dict:
    splits = jax.random.split(jax.random.key(seed), 7)
    return {
        "points": normal_values(splits[0], (TOKENS, D), 1.0, 6.0, ((0, 32),)),
        "order": jax.vmap(lambda own: jax.random.permutation(own, TOK_DEV))(jax.random.split(splits[1], DEVICES)).reshape((DEVICES, TOK_DEV)).astype(jnp.int32),
        "scan_ids": touch_ends(jax.random.randint(splits[2], (TOKENS,), 0, SCANS), jax.random.fold_in(splits[2], 1), 0, SCANS - 1).astype(jnp.int32),
        "ln_gain": jnp.clip(1.0 + 0.15 * jax.random.normal(splits[3], (2, D), jnp.float32), 0.25, 1.75),
        "w_qkv": draw_w_qkv(jax.random.fold_in(splits[6], 71), 0),
        "w_out": normal_values(splits[5], (2, D, D), D ** -0.5, 0.1875, ((1, 4),)),
    }


EPSILON = 1e-05

def layer_norm(rows, gain):
    values = rows.astype(jnp.float32)
    center = values - lax.optimization_barrier(jnp.mean(values, axis=-1, keepdims=True))
    spread = lax.optimization_barrier(jnp.mean(center * center, axis=-1, keepdims=True))
    return (center * lax.rsqrt(spread + EPSILON) * gain.astype(jnp.float32)).astype(jnp.bfloat16)

def window_attention(qkv_all, tags, offset):
    length = qkv_all.shape[0]
    rolled = jnp.roll(qkv_all, -offset, axis=0)
    rolled_tags = jnp.roll(tags, -offset, axis=0)
    windows = length // PATCH
    parts = rolled.reshape(windows, PATCH, HEADS, 3, HEAD_DIM)
    part_tags = rolled_tags.reshape(windows, PATCH)

    def one_window(inputs):
        piece, piece_tags = inputs
        queries = piece[:, :, 0].astype(jnp.float32)
        keys = piece[:, :, 1].astype(jnp.float32)
        values = piece[:, :, 2].astype(jnp.float32)
        scores = jnp.einsum('qhd,khd->hqk', queries, keys) * HEAD_DIM ** (-0.5)
        allowed = piece_tags[:, None] == piece_tags[None, :]
        scores = jnp.where(allowed[None], scores, -jnp.inf)
        row_max = lax.optimization_barrier(jnp.max(scores, axis=-1, keepdims=True))
        expo = jnp.exp(scores - row_max)
        probs = (expo / lax.optimization_barrier(jnp.sum(expo, axis=-1, keepdims=True))).astype(jnp.bfloat16)
        heads = jnp.einsum('hqk,khd->qhd', probs.astype(jnp.float32), values)
        return heads.astype(jnp.bfloat16)
    outputs = lax.map(one_window, (parts, part_tags))
    return jnp.roll(outputs.reshape(length, HEADS * HEAD_DIM), offset, axis=0)

def reference(points, order, scan_ids, ln_gain, w_qkv, w_out):
    blocks = points.reshape(-1, TOK_DEV, D)
    stream = jax.vmap(lambda block, picks: block[picks])(blocks, order.astype(jnp.int32)).reshape(-1, D)
    for layer_index in range(2):
        normed = layer_norm(stream, ln_gain[layer_index])
        qkv_all = jnp.dot(normed, w_qkv[layer_index], preferred_element_type=jnp.float32).astype(jnp.bfloat16)
        heads = window_attention(qkv_all, scan_ids, layer_index * (PATCH // 2))
        update = jnp.dot(heads, w_out[layer_index], preferred_element_type=jnp.float32)
        stream = (stream.astype(jnp.float32) + update).astype(jnp.bfloat16)
    return stream
```

```python
import functools

import jax
import jax.numpy as jnp
from jax import lax
from jax.experimental import pallas as pl
from jax.experimental.pallas import tpu as pltpu
from jax.sharding import PartitionSpec as P

HEAD_DIM = 64
PATCH = 1024


EPSILON = 1e-05


def layer_norm(rows, gain):
    values = rows.astype(jnp.float32)
    center = values - jnp.mean(values, axis=-1, keepdims=True)
    spread = jnp.mean(center * center, axis=-1, keepdims=True)
    return (center * lax.rsqrt(spread + EPSILON) * gain).astype(jnp.bfloat16)


def remote(src, dst, send_sem, recv_sem, device):
    return pltpu.make_async_remote_copy(
        src_ref=src,
        dst_ref=dst,
        send_sem=send_sem,
        recv_sem=recv_sem,
        device_id=device,
        device_id_type=pl.DeviceIdType.MESH,
    )


def layer_kernel(
    peers, ranges, halo, x_ref, tag_ref, w_ref, wo_ref, stream_ref, out_ref,
    all_x, q_buf, kv_buf, tags, att, heads, all_wo,
    x_recv, x_send, w_recv, w_send, t_recv, t_send, h_recv, h_send, kv_recv, kv_send,
):
    chunks, chunk_rows, _ = x_ref.shape
    rows = chunks * chunk_rows
    heads_local = w_ref.shape[1] // (3 * HEAD_DIM)
    chips = peers // 2
    window_blocks = PATCH // rows
    curve = lax.axis_index("curve")
    me = lax.axis_index("head")
    chip, core = me // 2, me % 2
    partner = chip * 2 + 1 - core
    up, down = {"curve": (curve + 1) % ranges}, {"curve": (curve + ranges - 1) % ranges}
    same = [((chip + s) % chips) * 2 + core for s in range(chips)]
    other = [((chip + s) % chips) * 2 + 1 - core for s in range(chips)]
    others = [(me + t) % peers for t in range(1, peers)]

    barrier = pltpu.get_barrier_semaphore()
    for blk in others:
        pl.semaphore_signal(
            barrier, inc=1, device_id={"head": blk}, device_id_type=pl.DeviceIdType.MESH
        )
    if halo:
        for neighbour in (up, down):
            pl.semaphore_signal(
                barrier, inc=1, device_id=neighbour, device_id_type=pl.DeviceIdType.MESH
            )
    pl.semaphore_wait(barrier, peers - 1 + (2 if halo else 0))

    def direct_x(s, c):
        dest = partner if s == 0 else same[s]
        return remote(
            x_ref.at[c], all_x.at[me, c], x_send.at[s, c], x_recv.at[me, c], {"head": dest}
        )

    def passed_x(s, c):
        part = all_x.at[same[s], c]
        return remote(
            part, part, x_send.at[chips + s, c], x_recv.at[same[s], c], {"head": partner}
        )

    def wait_x(blk, c):
        part = all_x.at[blk, c]
        remote(part, part, x_send.at[0, c], x_recv.at[blk, c], {"head": partner}).wait_recv()

    def tag_copy(t):
        return remote(
            tag_ref.at[0], tags.at[halo + me], t_send.at[t], t_recv.at[halo + me],
            {"head": others[t]},
        )

    def direct_w(s):
        dest = partner if s == 0 else same[s]
        return remote(wo_ref, all_wo.at[me], w_send.at[s], w_recv.at[me], {"head": dest})

    def passed_w(s):
        part = all_wo.at[same[s]]
        return remote(
            part, part, w_send.at[chips + s], w_recv.at[same[s]], {"head": partner}
        )

    def wait_w(blk):
        part = all_wo.at[blk]
        remote(part, part, w_send.at[0], w_recv.at[blk], {"head": partner}).wait_recv()

    def edge(buffer, send, recv, j):
        if j < halo:
            src, dst, device = buffer.at[peers + j], buffer.at[j], up
        else:
            src, dst, device = buffer.at[j], buffer.at[peers + j], down
        return remote(src, dst, send.at[j], recv.at[j], device)

    tag_send_edge = peers - 1

    for s in range(chips):
        for c in range(chunks):
            direct_x(s, c).start()
    for t in range(peers - 1):
        tag_copy(t).start()
    direct_w(0).start()
    tags[halo + me] = tag_ref[0]

    def project(values, blk, first_row):
        result = jnp.dot(values, w_ref[...], preferred_element_type=jnp.float32)
        result = result.astype(jnp.bfloat16)
        at = pl.ds(first_row, chunk_rows)
        for head in range(heads_local):
            base = head * 3 * HEAD_DIM
            q_buf[blk, at, head * HEAD_DIM : (head + 1) * HEAD_DIM] = result[
                :, base : base + HEAD_DIM
            ] * jnp.bfloat16(HEAD_DIM ** (-0.5))
            kv_buf[halo + blk, at, head * 2 * HEAD_DIM : (head + 1) * 2 * HEAD_DIM] = result[
                :, base + HEAD_DIM : base + 3 * HEAD_DIM
            ]

    def project_block(blk):
        for c in range(chunks):
            project(all_x[blk, c], blk, c * chunk_rows)

    def attend(blk):
        first = (blk + halo) // window_blocks * window_blocks
        column = jnp.transpose(
            jnp.broadcast_to(tags[halo + blk].astype(jnp.float32), (128, rows))
        )[:, :1]
        line = jnp.concatenate(
            [tags[first + j].astype(jnp.float32) for j in range(window_blocks)], axis=1
        )
        bias = jnp.where(column == line, 0.0, -jnp.inf)
        ones = jnp.ones((PATCH, HEAD_DIM), jnp.bfloat16)
        for head in range(heads_local):
            at = head * 2 * HEAD_DIM
            wide = kv_buf[pl.ds(first, window_blocks), :, at : at + 2 * HEAD_DIM].reshape(
                PATCH, 2 * HEAD_DIM
            )
            query = q_buf[blk, :, head * HEAD_DIM : (head + 1) * HEAD_DIM]
            scores = lax.dot_general(
                query, wide[:, :HEAD_DIM], (((1,), (1,)), ((), ())),
                preferred_element_type=jnp.float32,
            ) + bias
            row_max = jnp.max(scores, axis=-1, keepdims=True)
            expo = jnp.exp(scores - row_max).astype(jnp.bfloat16)
            result = jnp.dot(
                expo,
                jnp.concatenate([wide[:, HEAD_DIM:], ones], axis=1),
                preferred_element_type=jnp.float32,
            )
            normal = result[:, :HEAD_DIM] / result[:, HEAD_DIM : HEAD_DIM + 1]
            att[blk, :, head * HEAD_DIM : (head + 1) * HEAD_DIM] = normal.astype(jnp.bfloat16)

    def head_copy(t):
        blk = others[t]
        return remote(
            att.at[blk], heads.at[me], h_send.at[t], h_recv.at[me], {"head": blk}
        )

    def head_copy_to(blk):
        t = (blk - me + peers - 1) % peers
        return remote(
            att.at[blk], heads.at[me], h_send.at[t], h_recv.at[me], {"head": blk}
        )

    for c in range(chunks):
        project(x_ref[c], me, c * chunk_rows)
    for c in range(chunks):
        wait_x(partner, c)
    project_block(partner)
    for blk in others:
        part = tags.at[halo + blk]
        remote(part, part, t_send.at[0], t_recv.at[halo + blk], {"head": partner}).wait_recv()
    if halo:
        for j in range(2 * halo):
            edge(tags, t_send.at[pl.ds(peers, 2 * halo)], t_recv.at[pl.ds(peers + 2 * halo, 2 * halo)], j).start()

    early = not halo and window_blocks == 2
    if early:
        attend(me)
        attend(partner)
        head_copy_to(partner).start()
    for s in range(1, chips):
        for c in range(chunks):
            wait_x(same[s], c)
            passed_x(s, c).start()
            project(all_x[same[s], c], same[s], c * chunk_rows)
    for s in range(1, chips):
        direct_w(s).start()
        for c in range(chunks):
            wait_x(other[s], c)
            project(all_x[other[s], c], other[s], c * chunk_rows)
    if halo:
        for j in range(2 * halo):
            edge(kv_buf, kv_send, kv_recv, j).start()
        middle = chips // 2 if window_blocks == 2 else 0
        for j in range(2 * halo):
            edge(tags, t_send.at[pl.ds(peers, 2 * halo)], t_recv.at[pl.ds(peers + 2 * halo, 2 * halo)], j).wait_recv()

    def finish(blk):
        attend(blk)

        @pl.when(blk != me)
        def _():
            head_copy_to(blk).start()

    if early:
        for s in range(1, chips):
            finish(other[s])
            finish(same[s])
    else:
        if halo:
            inner = list(range(halo, peers - halo))
            outer = list(range(peers - halo, peers)) + list(range(halo))

            def inner_step(i, carry):
                finish(halo + (me + 1 + i) % (peers - 2 * halo))
                return carry

            lax.fori_loop(0, len(inner), inner_step, 0)
            for j in range(2 * halo):
                edge(kv_buf, kv_send, kv_recv, j).wait_recv()

            def outer_step(i, carry):
                finish((peers - halo + (me + i) % (2 * halo)) % peers)
                return carry

            lax.fori_loop(0, len(outer), outer_step, 0)
        else:

            def step(i, carry):
                finish((me + 1 + i) % peers)
                return carry

            lax.fori_loop(0, peers, step, 0)

    wait_w(partner)
    for s in range(1, chips):
        wait_w(same[s])
        passed_w(s).start()
    heads[me] = att[me]
    all_wo[me] = wo_ref[...]
    for s in range(1, chips):
        wait_w(other[s])
    for blk in others:
        part = heads.at[blk]
        remote(part, part, h_send.at[0], h_recv.at[blk], {"head": partner}).wait_recv()

    for c in range(chunks):
        at = pl.ds(c * chunk_rows, chunk_rows)
        total = stream_ref[at, :].astype(jnp.float32)
        for blk in range(peers):
            total += jnp.dot(
                heads[blk, at, :], all_wo[blk], preferred_element_type=jnp.float32
            )
        out_ref[at, :] = total.astype(jnp.bfloat16)

    for s in range(chips):
        for c in range(chunks):
            direct_x(s, c).wait_send()
            if s:
                passed_x(s, c).wait_send()
        direct_w(s).wait_send()
        if s:
            passed_w(s).wait_send()
    for t in range(peers - 1):
        tag_copy(t).wait_send()
        head_copy(t).wait_send()
    for j in range(2 * halo):
        edge(tags, t_send.at[pl.ds(peers, 2 * halo)], t_recv.at[pl.ds(peers + 2 * halo, 2 * halo)], j).wait_send()
        edge(kv_buf, kv_send, kv_recv, j).wait_send()


def layer(index, stream, normed, tag_row, weights, out_weights):
    rows, width = stream.shape
    peers, ranges = lax.axis_size("head"), lax.axis_size("curve")
    halo = PATCH // 2 // rows if index else 0
    chips = peers // 2
    chunks = max(1, rows // 256)
    columns = out_weights.shape[0]
    vmem = pl.BlockSpec(memory_space=pltpu.VMEM)
    dma = pltpu.SemaphoreType.DMA
    bf16 = jnp.bfloat16
    return pl.pallas_call(
        functools.partial(layer_kernel, peers, ranges, halo),
        out_shape=jax.ShapeDtypeStruct((rows, width), bf16),
        in_specs=[vmem] * 5,
        out_specs=vmem,
        scratch_shapes=[
            pltpu.VMEM((peers, chunks, rows // chunks, width), bf16),
            pltpu.VMEM((peers, rows, columns), bf16),
            pltpu.VMEM((peers + 2 * halo, rows, 2 * columns), bf16),
            pltpu.VMEM((peers + 2 * halo, 1, rows), jnp.int32),
            pltpu.VMEM((peers, rows, columns), bf16),
            pltpu.VMEM((peers, rows, columns), bf16),
            pltpu.VMEM((peers, columns, width), bf16),
            dma((peers, chunks)),
            dma((peers, chunks)),
            dma((peers,)),
            dma((peers,)),
            dma((peers + 4 * halo,)),
            dma((peers + 2 * halo,)),
            dma((peers,)),
            dma((peers,)),
            dma((max(1, 2 * halo),)),
            dma((max(1, 2 * halo),)),
        ],
        compiler_params=pltpu.CompilerParams(collective_id=index, has_side_effects=True),
        cost_estimate=pl.CostEstimate(
            flops=20 * rows * width * width, bytes_accessed=20 * rows * width, transcendentals=0
        ),
    )(
        normed.reshape(chunks, rows // chunks, width),
        tag_row,
        weights,
        out_weights,
        stream,
    )


SCANS = 4
BLOCKED = -1e30
LOG2_SCALE = 1.4426950408889634 * HEAD_DIM ** (-0.5)
LANES = 128


def pieces(index, extent):
    alone = extent // 8 if index == 0 else 0
    return alone, (extent - 2 * alone) // 4


def fused_kernel(
    peers, ranges,
    points_ref, order_ref, tag_ref, gain_ref, wq_hbm, wo_hbm, out_ref,
    xs, stream, wq, wo, query, keys, values, att, acc, peak, tags, tag_q, tag_k,
    send_sem, recv_sem, load_sem,
):
    rows, width = points_ref.shape
    layers, steps, _, columns = wq.shape
    depth = wo_hbm.shape[1]
    curve = lax.axis_index("curve")
    me = lax.axis_index("head")
    chip, core = me // 2, me % 2
    x_at, z_at = curve % 2, curve // 2 % 2
    partner = {"head": chip * 2 + 1 - core}
    across = {"head": (me + 2) % peers}
    beside = {"curve": curve + 1 - 2 * x_at}
    above = {"curve": curve + 2 - 4 * z_at}
    total = peers * ranges
    block = (curve * peers + me + 2 * core - 1 + total) % total
    pair = {"curve": block // peers, "head": block % peers}

    bf16, f32 = jnp.bfloat16, jnp.float32
    lane = lax.broadcasted_iota(jnp.int32, (1, LANES), 1)
    low = lane < HEAD_DIM
    numbers, order_of_sends = {}, []

    def number(key):
        return numbers.setdefault(key, len(numbers))

    def copy(key, src, dst, device):
        at = number(key)
        return remote(src, dst, send_sem.at[at], recv_sem.at[at], device)

    def send(key, src, dst, device):
        order_of_sends.append((key, src, dst, device))
        copy(key, src, dst, device).start()

    def arrive(key, part):
        copy(key, part, part, partner).wait_recv()

    barrier = pltpu.get_barrier_semaphore()
    for device in (partner, across, beside, above, pair):
        pl.semaphore_signal(
            barrier, inc=1, device_id=device, device_id_type=pl.DeviceIdType.MESH
        )

    loads = []
    for index in range(layers):
        for p in range(2):
            loads.append((wq_hbm.at[index, :, pl.ds(p * columns, columns)], wq.at[index, p]))
        loads.append((wo_hbm.at[index], wo.at[index, 0]))

    def load(n):
        return pltpu.make_async_copy(loads[n][0], loads[n][1], load_sem.at[n])

    for n in range(len(loads)):
        load(n).start()

    def home(index, chunk):
        if chunk < 2:
            return wq_hbm.at[index, :, pl.ds(chunk * columns, columns)], wq.at[index, 4 + 2 * chunk]
        return wo_hbm.at[index], wo.at[index, 2]

    def extent(chunk):
        return width if chunk < 2 else depth

    def cut(index, chunk, kind):
        alone, shared = pieces(index, extent(chunk))
        cuts = 2 if chunk < 2 else 1
        size = alone if kind[0] == "a" else shared
        if not size:
            return []
        x_of = x_at if kind[1] == "s" else 1 - x_at
        if kind[0] == "a":
            base = x_of * alone
        else:
            z_of = z_at if kind[2] == "s" else 1 - z_at
            base = 2 * alone + (x_of * 2 + z_of) * shared
        size //= cuts
        return [pl.ds(pl.multiple_of(base + c * size, 16), size) for c in range(cuts)]

    kinds = ("qss", "qso", "qos", "qoo", "as", "ao")
    every = [(index, chunk) for index in range(layers) for chunk in range(3)]
    homes = {which: home(*which) for which in every}
    theres = {
        (index, chunk): wq.at[index, 5 + 2 * chunk] if chunk < 2 else wo.at[index, 3]
        for index, chunk in every
    }
    parts_of = {
        (*which, kind): [homes[which][1].at[at] for at in cut(*which, kind)]
        for which in every
        for kind in kinds
    }

    def first(index, chunk):
        source, _ = homes[index, chunk]
        for kind in ("qss", "as"):
            for c, at in enumerate(cut(index, chunk, kind)):
                part = parts_of[index, chunk, kind][c]
                send(("y", index, chunk, kind, c), source.at[at], part, across)

    def second(index, chunk):
        for c, part in enumerate(parts_of[index, chunk, "qss"]):
            arrive(("y", index, chunk, "qss", c), part)
            send(("x", index, chunk, "q", c), part, part, beside)
            send(("z", index, chunk, "s", c), part, part, above)

    def third(index, chunk):
        for c, part in enumerate(parts_of[index, chunk, "as"]):
            arrive(("y", index, chunk, "as", c), part)
            send(("x", index, chunk, "a", c), part, part, beside)
        for c, part in enumerate(parts_of[index, chunk, "qos"]):
            arrive(("x", index, chunk, "q", c), part)
            send(("z", index, chunk, "o", c), part, part, above)

    def fourth(index, chunk):
        for c, part in enumerate(parts_of[index, chunk, "ao"]):
            arrive(("x", index, chunk, "a", c), part)
        for c, part in enumerate(parts_of[index, chunk, "qso"]):
            arrive(("z", index, chunk, "s", c), part)
        for c, part in enumerate(parts_of[index, chunk, "qoo"]):
            arrive(("z", index, chunk, "o", c), part)
        send(("f", index, chunk), homes[index, chunk][1], theres[index, chunk], partner)

    def fifth(index, chunk):
        arrive(("f", index, chunk), theres[index, chunk])

    def share(index, chunk):
        source, _ = home(index, chunk)
        there = wq.at[index, 2 + chunk] if chunk < 2 else wo.at[index, 1]
        send(("w", index, chunk), source, there, partner)

    def shared(index, chunk):
        there = wq.at[index, 2 + chunk] if chunk < 2 else wo.at[index, 1]
        arrive(("w", index, chunk), there)

    def column_of(row):
        return jnp.transpose(jnp.broadcast_to(row.astype(f32), (LANES, row.shape[1])))

    def key_tags(slot):
        spot = (lane % HEAD_DIM).astype(f32)
        return jnp.where(column_of(tags[slot]) == spot, BLOCKED, 0.0)

    half = rows // 2

    def normed(index, part):
        at = pl.ds(part * half, half)
        xs[index, 0, at, :] = layer_norm(
            stream[at, :].astype(f32), gain_ref[index : index + 1, :]
        )

    def exchange(index, part):
        at = pl.ds(part * half, half)
        send(
            ("n", index, part), xs.at[index, 0, at], xs.at[index, 1, at],
            pair if index else partner,
        )

    def exchanged(index, part):
        arrive(("n", index, part), xs.at[index, 1, pl.ds(part * half, half)])

    column = column_of(order_ref[...])[:, :1]
    picks = (column == lax.broadcasted_iota(jnp.int32, (1, rows), 1).astype(f32)).astype(bf16)
    stream[...] = jnp.dot(picks, points_ref[...], preferred_element_type=f32).astype(bf16)
    normed(0, 0)
    normed(0, 1)
    tags[0] = tag_ref[...]
    spot = (lane % HEAD_DIM).astype(f32)
    own = column_of(tag_ref[...])
    tag_q[...] = jnp.where((spot < SCANS) & (own != spot), 1.0, 0.0)
    tag_k[0] = key_tags(0)

    pl.semaphore_wait(barrier, 5)
    first(0, 0)
    send(("t", 0), tag_ref, tags.at[1], partner)
    send(("t", 1), tag_ref, tags.at[2], pair)
    exchange(0, 0)
    exchange(0, 1)
    first(0, 1)
    first(0, 2)
    for index in range(layers):
        for chunk in range(3):
            share(index, chunk)
    for chunk in range(3):
        first(1, chunk)

    def project(index, k, side, q_at):
        result = jnp.dot(xs[index, side], wq[index, k], preferred_element_type=f32)
        left, middle, right = (result[:, LANES * n : LANES * (n + 1)] for n in range(3))
        at = pl.ds(side * rows, rows)
        marks = tag_k[side]
        keys[0, at, :] = jnp.where(low, marks, left).astype(bf16)
        values[0, at, :] = jnp.where(low, middle, 1.0).astype(bf16)
        keys[1, at, :] = jnp.where(low, right, marks).astype(bf16)
        values[1, at, :] = jnp.where(low, 1.0, right).astype(bf16)
        if side == 0:
            marks = tag_q[...]
            query[q_at, 0] = jnp.where(
                low, marks, pltpu.roll(left * LOG2_SCALE, HEAD_DIM, 1)
            ).astype(bf16)
            query[q_at, 1] = jnp.where(
                low, pltpu.roll(middle * LOG2_SCALE, HEAD_DIM, 1), marks
            ).astype(bf16)

    def scores(q_at, head, at, over):
        return lax.dot_general(
            query[q_at, head, at, :], keys[head, over, :], (((1,), (1,)), ((), ())),
            preferred_element_type=f32,
        )

    def settle(k, at, sums):
        parts = [s / pltpu.roll(s, HEAD_DIM, 1) for s in sums]
        att[k, at, :] = jnp.where(low, parts[0], parts[1]).astype(bf16)

    row_blocks = [pl.ds(r * (rows // 2), rows // 2) for r in range(2)]

    def attend(k):
        for at in row_blocks:
            sums = []
            for head in range(2):
                table = scores(0, head, at, slice(None))
                top = jnp.max(table, axis=-1, keepdims=True)
                expo = jnp.exp2(table - top).astype(bf16)
                sums.append(jnp.dot(expo, values[head], preferred_element_type=f32))
            settle(k, at, sums)

    def attend_own(k):
        over = pl.ds(0, rows)
        for at in row_blocks:
            for head in range(2):
                table = scores(k, head, at, over)
                top = jnp.max(table, axis=-1, keepdims=True)
                expo = jnp.exp2(table - top).astype(bf16)
                acc[k, head, at, :] = jnp.dot(
                    expo, values[head, over, :], preferred_element_type=f32
                )
                peak[k, head, at, :] = jnp.broadcast_to(top, (rows // 2, LANES))

    def attend_pair(k):
        over = pl.ds(rows, rows)
        for at in row_blocks:
            sums = []
            for head in range(2):
                table = scores(k, head, at, over)
                before = peak[k, head, at, :]
                top = jnp.maximum(before[:, :1], jnp.max(table, axis=-1, keepdims=True))
                expo = jnp.exp2(table - top).astype(bf16)
                sums.append(
                    jnp.dot(expo, values[head, over, :], preferred_element_type=f32)
                    + acc[k, head, at, :] * jnp.exp2(before - top)
                )
            settle(k, at, sums)

    def leave(index, part):
        at = pl.ds(part * half, half)
        result = stream[at, :].astype(f32)
        for slot, (one, two) in enumerate(((0, 1), (2, 3), (4, 6), (5, 7))):
            result += jnp.dot(
                jnp.concatenate([att[one, at, :], att[two, at, :]], axis=1),
                wo[index, slot],
                preferred_element_type=f32,
            )
        return result.astype(bf16)

    def run(events, body):
        def step(k, carry):
            for when, todo in events.items():
                @pl.when(k == when)
                def _(todo=todo):
                    for event, args in todo:
                        event(*args)
            body(k)
            return carry

        lax.fori_loop(0, steps, step, 0)

    arrive(("t", 0), tags.at[1])
    tag_k[1] = key_tags(1)
    exchanged(0, 0)
    exchanged(0, 1)

    def whole(k):
        project(0, k, 0, 0)
        project(0, k, 1, 0)
        attend(k)

    def loaded(n):
        load(n).wait()

    run(
        {
            0: [(loaded, (0,)), (loaded, (1,))],
            1: [(second, (0, 0))],
            2: [(shared, (0, 0)), (third, (0, 0))],
            3: [(shared, (0, 1)), (second, (0, 1))],
            4: [(fourth, (0, 0)), (third, (0, 1)), (second, (0, 2))],
            5: [(third, (0, 2)), (fifth, (0, 0))],
            6: [(fourth, (0, 1)), (second, (1, 0))],
            7: [(fourth, (0, 2)), (third, (1, 0)), (fifth, (0, 1))],
        },
        whole,
    )
    loaded(2)
    shared(0, 2)
    fifth(0, 2)
    for part in range(2):
        at = pl.ds(part * half, half)
        stream[at, :] = leave(0, part)
        normed(1, part)
        exchange(1, part)
    second(1, 1)
    arrive(("t", 1), tags.at[2])
    tag_k[1] = key_tags(2)

    def inner(k):
        project(1, k, 0, k)
        attend_own(k)

    run(
        {
            0: [(loaded, (3,)), (loaded, (4,))],
            1: [(third, (1, 1))],
            2: [(shared, (1, 0)), (fourth, (1, 0))],
            3: [(shared, (1, 1)), (second, (1, 2))],
            5: [(fifth, (1, 0)), (third, (1, 2))],
            6: [(fourth, (1, 1))],
            7: [(fifth, (1, 1))],
        },
        inner,
    )
    fourth(1, 2)
    exchanged(1, 0)
    exchanged(1, 1)

    def outer(k):
        project(1, k, 1, k)
        attend_pair(k)

    run({}, outer)
    loaded(5)
    shared(1, 2)
    fifth(1, 2)
    for part in range(2):
        out_ref[pl.ds(part * half, half), :] = leave(1, part)

    for key, src, dst, device in order_of_sends:
        copy(key, src, dst, device).wait_send()


def fused(points, order, scan_ids, ln_gain, w_qkv, w_out):
    rows, width = points.shape
    peers, ranges = lax.axis_size("head"), lax.axis_size("curve")
    layers, _, columns = w_qkv.shape
    columns //= 2
    steps = 2 * peers
    vmem, far = pl.BlockSpec(memory_space=pltpu.VMEM), pl.BlockSpec(memory_space=pl.ANY)
    dma = pltpu.SemaphoreType.DMA
    bf16, f32 = jnp.bfloat16, jnp.float32
    return pl.pallas_call(
        functools.partial(fused_kernel, peers, ranges),
        out_shape=jax.ShapeDtypeStruct((rows, width), bf16),
        in_specs=[vmem] * 4 + [far] * 2,
        out_specs=vmem,
        scratch_shapes=[
            pltpu.VMEM((layers, 2, rows, width), bf16),
            pltpu.VMEM((rows, width), bf16),
            pltpu.VMEM((layers, steps, width, columns), bf16),
            pltpu.VMEM((layers, peers, width // peers, width), bf16),
            pltpu.VMEM((steps, 2, rows, LANES), bf16),
            pltpu.VMEM((2, 2 * rows, LANES), bf16),
            pltpu.VMEM((2, 2 * rows, LANES), bf16),
            pltpu.VMEM((steps, rows, LANES), bf16),
            pltpu.VMEM((steps, 2, rows, LANES), f32),
            pltpu.VMEM((steps, 2, rows, LANES), f32),
            pltpu.VMEM((3, 1, rows), jnp.int32),
            pltpu.VMEM((rows, LANES), f32),
            pltpu.VMEM((2, rows, LANES), f32),
            dma((96,)),
            dma((96,)),
            dma((3 * layers,)),
        ],
        compiler_params=pltpu.CompilerParams(
            collective_id=0, has_side_effects=True, vmem_limit_bytes=60 * 1024 * 1024
        ),
        cost_estimate=pl.CostEstimate(
            flops=80 * rows * width * width, bytes_accessed=20 * rows * width, transcendentals=0
        ),
    )(points, order, scan_ids.reshape(1, -1), ln_gain, w_qkv, w_out)


def chip_holds_window(points, w_qkv):
    peers, ranges = lax.axis_size("head"), lax.axis_size("curve")
    rows, width = points.shape
    return (
        peers == 4
        and ranges % 4 == 0
        and PATCH == 2 * rows
        and w_qkv.shape[0] == 2
        and w_qkv.shape[2] == 12 * HEAD_DIM
        and width == peers * 4 * HEAD_DIM
    )


def on_device(points, order, scan_ids, ln_gain, w_qkv, w_out):
    if chip_holds_window(points, w_qkv):
        return fused(points, order, scan_ids, ln_gain, w_qkv, w_out)
    stream = points[order[0]]
    tag_row = scan_ids.reshape(1, 1, -1)
    for index in range(2):
        normed = layer_norm(stream, ln_gain[index])
        stream = layer(index, stream, normed, tag_row, w_qkv[index], w_out[index])
    return stream


def solution(mesh):
    in_specs = (
        P(("curve", "head"), None),
        P(("curve", "head"), None),
        P(("curve", "head")),
        P(),
        P(None, None, "head"),
        P(None, "head", None),
    )
    out_specs = P(("curve", "head"), None)
    return jax.shard_map(
        on_device, mesh=mesh, in_specs=in_specs, out_specs=out_specs, check_vma=False
    )
```

```python
import functools

import jax
import jax.numpy as jnp
from jax import lax
from jax.experimental import pallas as pl
from jax.experimental.pallas import tpu as pltpu
from jax.sharding import PartitionSpec as P

HEAD_DIM = 64
PATCH = 1024


EPSILON = 1e-05


def layer_norm(rows, gain):
    values = rows.astype(jnp.float32)
    center = values - jnp.mean(values, axis=-1, keepdims=True)
    spread = jnp.mean(center * center, axis=-1, keepdims=True)
    return (center * lax.rsqrt(spread + EPSILON) * gain).astype(jnp.bfloat16)


def remote(src, dst, send_sem, recv_sem, device):
    return pltpu.make_async_remote_copy(
        src_ref=src,
        dst_ref=dst,
        send_sem=send_sem,
        recv_sem=recv_sem,
        device_id=device,
        device_id_type=pl.DeviceIdType.MESH,
    )


def layer_kernel(
    peers, ranges, halo, x_ref, tag_ref, w_ref, wo_ref, stream_ref, out_ref,
    all_x, q_buf, kv_buf, tags, att, heads, all_wo,
    x_recv, x_send, w_recv, w_send, t_recv, t_send, h_recv, h_send, kv_recv, kv_send,
):
    chunks, chunk_rows, _ = x_ref.shape
    rows = chunks * chunk_rows
    heads_local = w_ref.shape[1] // (3 * HEAD_DIM)
    chips = peers // 2
    window_blocks = PATCH // rows
    curve = lax.axis_index("curve")
    me = lax.axis_index("head")
    chip, core = me // 2, me % 2
    partner = chip * 2 + 1 - core
    up, down = {"curve": (curve + 1) % ranges}, {"curve": (curve + ranges - 1) % ranges}
    same = [((chip + s) % chips) * 2 + core for s in range(chips)]
    other = [((chip + s) % chips) * 2 + 1 - core for s in range(chips)]
    others = [(me + t) % peers for t in range(1, peers)]

    barrier = pltpu.get_barrier_semaphore()
    for blk in others:
        pl.semaphore_signal(
            barrier, inc=1, device_id={"head": blk}, device_id_type=pl.DeviceIdType.MESH
        )
    if halo:
        for neighbour in (up, down):
            pl.semaphore_signal(
                barrier, inc=1, device_id=neighbour, device_id_type=pl.DeviceIdType.MESH
            )
    pl.semaphore_wait(barrier, peers - 1 + (2 if halo else 0))

    def direct_x(s, c):
        dest = partner if s == 0 else same[s]
        return remote(
            x_ref.at[c], all_x.at[me, c], x_send.at[s, c], x_recv.at[me, c], {"head": dest}
        )

    def passed_x(s, c):
        part = all_x.at[same[s], c]
        return remote(
            part, part, x_send.at[chips + s, c], x_recv.at[same[s], c], {"head": partner}
        )

    def wait_x(blk, c):
        part = all_x.at[blk, c]
        remote(part, part, x_send.at[0, c], x_recv.at[blk, c], {"head": partner}).wait_recv()

    def tag_copy(t):
        return remote(
            tag_ref.at[0], tags.at[halo + me], t_send.at[t], t_recv.at[halo + me],
            {"head": others[t]},
        )

    def direct_w(s):
        dest = partner if s == 0 else same[s]
        return remote(wo_ref, all_wo.at[me], w_send.at[s], w_recv.at[me], {"head": dest})

    def passed_w(s):
        part = all_wo.at[same[s]]
        return remote(
            part, part, w_send.at[chips + s], w_recv.at[same[s]], {"head": partner}
        )

    def wait_w(blk):
        part = all_wo.at[blk]
        remote(part, part, w_send.at[0], w_recv.at[blk], {"head": partner}).wait_recv()

    def edge(buffer, send, recv, j):
        if j < halo:
            src, dst, device = buffer.at[peers + j], buffer.at[j], up
        else:
            src, dst, device = buffer.at[j], buffer.at[peers + j], down
        return remote(src, dst, send.at[j], recv.at[j], device)

    tag_send_edge = peers - 1

    for s in range(chips):
        for c in range(chunks):
            direct_x(s, c).start()
    for t in range(peers - 1):
        tag_copy(t).start()
    direct_w(0).start()
    tags[halo + me] = tag_ref[0]

    def project(values, blk, first_row):
        result = jnp.dot(values, w_ref[...], preferred_element_type=jnp.float32)
        result = result.astype(jnp.bfloat16)
        at = pl.ds(first_row, chunk_rows)
        for head in range(heads_local):
            base = head * 3 * HEAD_DIM
            q_buf[blk, at, head * HEAD_DIM : (head + 1) * HEAD_DIM] = result[
                :, base : base + HEAD_DIM
            ] * jnp.bfloat16(HEAD_DIM ** (-0.5))
            kv_buf[halo + blk, at, head * 2 * HEAD_DIM : (head + 1) * 2 * HEAD_DIM] = result[
                :, base + HEAD_DIM : base + 3 * HEAD_DIM
            ]

    def project_block(blk):
        for c in range(chunks):
            project(all_x[blk, c], blk, c * chunk_rows)

    def attend(blk):
        first = (blk + halo) // window_blocks * window_blocks
        column = jnp.transpose(
            jnp.broadcast_to(tags[halo + blk].astype(jnp.float32), (128, rows))
        )[:, :1]
        line = jnp.concatenate(
            [tags[first + j].astype(jnp.float32) for j in range(window_blocks)], axis=1
        )
        bias = jnp.where(column == line, 0.0, -jnp.inf)
        ones = jnp.ones((PATCH, HEAD_DIM), jnp.bfloat16)
        for head in range(heads_local):
            at = head * 2 * HEAD_DIM
            wide = kv_buf[pl.ds(first, window_blocks), :, at : at + 2 * HEAD_DIM].reshape(
                PATCH, 2 * HEAD_DIM
            )
            query = q_buf[blk, :, head * HEAD_DIM : (head + 1) * HEAD_DIM]
            scores = lax.dot_general(
                query, wide[:, :HEAD_DIM], (((1,), (1,)), ((), ())),
                preferred_element_type=jnp.float32,
            ) + bias
            row_max = jnp.max(scores, axis=-1, keepdims=True)
            expo = jnp.exp(scores - row_max).astype(jnp.bfloat16)
            result = jnp.dot(
                expo,
                jnp.concatenate([wide[:, HEAD_DIM:], ones], axis=1),
                preferred_element_type=jnp.float32,
            )
            normal = result[:, :HEAD_DIM] / result[:, HEAD_DIM : HEAD_DIM + 1]
            att[blk, :, head * HEAD_DIM : (head + 1) * HEAD_DIM] = normal.astype(jnp.bfloat16)

    def head_copy(t):
        blk = others[t]
        return remote(
            att.at[blk], heads.at[me], h_send.at[t], h_recv.at[me], {"head": blk}
        )

    def head_copy_to(blk):
        t = (blk - me + peers - 1) % peers
        return remote(
            att.at[blk], heads.at[me], h_send.at[t], h_recv.at[me], {"head": blk}
        )

    for c in range(chunks):
        project(x_ref[c], me, c * chunk_rows)
    for c in range(chunks):
        wait_x(partner, c)
    project_block(partner)
    for blk in others:
        part = tags.at[halo + blk]
        remote(part, part, t_send.at[0], t_recv.at[halo + blk], {"head": partner}).wait_recv()
    if halo:
        for j in range(2 * halo):
            edge(tags, t_send.at[pl.ds(peers, 2 * halo)], t_recv.at[pl.ds(peers + 2 * halo, 2 * halo)], j).start()

    early = not halo and window_blocks == 2
    if early:
        attend(me)
        attend(partner)
        head_copy_to(partner).start()
    for s in range(1, chips):
        for c in range(chunks):
            wait_x(same[s], c)
            passed_x(s, c).start()
            project(all_x[same[s], c], same[s], c * chunk_rows)
    for s in range(1, chips):
        direct_w(s).start()
        for c in range(chunks):
            wait_x(other[s], c)
            project(all_x[other[s], c], other[s], c * chunk_rows)
    if halo:
        for j in range(2 * halo):
            edge(kv_buf, kv_send, kv_recv, j).start()
        middle = chips // 2 if window_blocks == 2 else 0
        for j in range(2 * halo):
            edge(tags, t_send.at[pl.ds(peers, 2 * halo)], t_recv.at[pl.ds(peers + 2 * halo, 2 * halo)], j).wait_recv()

    def finish(blk):
        attend(blk)

        @pl.when(blk != me)
        def _():
            head_copy_to(blk).start()

    if early:
        for s in range(1, chips):
            finish(other[s])
            finish(same[s])
    else:
        if halo:
            inner = list(range(halo, peers - halo))
            outer = list(range(peers - halo, peers)) + list(range(halo))

            def inner_step(i, carry):
                finish(halo + (me + 1 + i) % (peers - 2 * halo))
                return carry

            lax.fori_loop(0, len(inner), inner_step, 0)
            for j in range(2 * halo):
                edge(kv_buf, kv_send, kv_recv, j).wait_recv()

            def outer_step(i, carry):
                finish((peers - halo + (me + i) % (2 * halo)) % peers)
                return carry

            lax.fori_loop(0, len(outer), outer_step, 0)
        else:

            def step(i, carry):
                finish((me + 1 + i) % peers)
                return carry

            lax.fori_loop(0, peers, step, 0)

    wait_w(partner)
    for s in range(1, chips):
        wait_w(same[s])
        passed_w(s).start()
    heads[me] = att[me]
    all_wo[me] = wo_ref[...]
    for s in range(1, chips):
        wait_w(other[s])
    for blk in others:
        part = heads.at[blk]
        remote(part, part, h_send.at[0], h_recv.at[blk], {"head": partner}).wait_recv()

    for c in range(chunks):
        at = pl.ds(c * chunk_rows, chunk_rows)
        total = stream_ref[at, :].astype(jnp.float32)
        for blk in range(peers):
            total += jnp.dot(
                heads[blk, at, :], all_wo[blk], preferred_element_type=jnp.float32
            )
        out_ref[at, :] = total.astype(jnp.bfloat16)

    for s in range(chips):
        for c in range(chunks):
            direct_x(s, c).wait_send()
            if s:
                passed_x(s, c).wait_send()
        direct_w(s).wait_send()
        if s:
            passed_w(s).wait_send()
    for t in range(peers - 1):
        tag_copy(t).wait_send()
        head_copy(t).wait_send()
    for j in range(2 * halo):
        edge(tags, t_send.at[pl.ds(peers, 2 * halo)], t_recv.at[pl.ds(peers + 2 * halo, 2 * halo)], j).wait_send()
        edge(kv_buf, kv_send, kv_recv, j).wait_send()


def layer(index, stream, normed, tag_row, weights, out_weights):
    rows, width = stream.shape
    peers, ranges = lax.axis_size("head"), lax.axis_size("curve")
    halo = PATCH // 2 // rows if index else 0
    chips = peers // 2
    chunks = max(1, rows // 256)
    columns = out_weights.shape[0]
    vmem = pl.BlockSpec(memory_space=pltpu.VMEM)
    dma = pltpu.SemaphoreType.DMA
    bf16 = jnp.bfloat16
    return pl.pallas_call(
        functools.partial(layer_kernel, peers, ranges, halo),
        out_shape=jax.ShapeDtypeStruct((rows, width), bf16),
        in_specs=[vmem] * 5,
        out_specs=vmem,
        scratch_shapes=[
            pltpu.VMEM((peers, chunks, rows // chunks, width), bf16),
            pltpu.VMEM((peers, rows, columns), bf16),
            pltpu.VMEM((peers + 2 * halo, rows, 2 * columns), bf16),
            pltpu.VMEM((peers + 2 * halo, 1, rows), jnp.int32),
            pltpu.VMEM((peers, rows, columns), bf16),
            pltpu.VMEM((peers, rows, columns), bf16),
            pltpu.VMEM((peers, columns, width), bf16),
            dma((peers, chunks)),
            dma((peers, chunks)),
            dma((peers,)),
            dma((peers,)),
            dma((peers + 4 * halo,)),
            dma((peers + 2 * halo,)),
            dma((peers,)),
            dma((peers,)),
            dma((max(1, 2 * halo),)),
            dma((max(1, 2 * halo),)),
        ],
        compiler_params=pltpu.CompilerParams(collective_id=index, has_side_effects=True),
        cost_estimate=pl.CostEstimate(
            flops=20 * rows * width * width, bytes_accessed=20 * rows * width, transcendentals=0
        ),
    )(
        normed.reshape(chunks, rows // chunks, width),
        tag_row,
        weights,
        out_weights,
        stream,
    )


SCANS = 4
BLOCKED = -1e30
LOG2_SCALE = 1.4426950408889634 * HEAD_DIM ** (-0.5)
LANES = 128


def pieces(index, extent):
    alone = extent // 8
    return alone, (extent - 2 * alone) // 4


def fused_kernel(
    peers, ranges,
    points_ref, order_ref, tag_ref, gain_ref, wq_hbm, wo_hbm, out_ref,
    xs, stream, wq, wo, query, keys, values, att, acc, peak, tags, tag_q, tag_k,
    given, send_sem, recv_sem, load_sem, given_send, given_recv,
):
    rows, width = points_ref.shape
    layers, steps, _, columns = wq.shape
    depth = wo_hbm.shape[1]
    curve = lax.axis_index("curve")
    me = lax.axis_index("head")
    chip, core = me // 2, me % 2
    x_at, z_at = curve % 2, curve // 2 % 2
    partner = {"head": chip * 2 + 1 - core}
    across = {"head": (me + 2) % peers}
    beside = {"curve": curve + 1 - 2 * x_at}
    above = {"curve": curve + 2 - 4 * z_at}
    total = peers * ranges
    block = (curve * peers + me + 2 * core - 1 + total) % total
    pair = {"curve": block // peers, "head": block % peers}

    bf16, f32 = jnp.bfloat16, jnp.float32
    lane = lax.broadcasted_iota(jnp.int32, (1, LANES), 1)
    low = lane < HEAD_DIM
    numbers, order_of_sends = {}, []

    def number(key):
        return numbers.setdefault(key, len(numbers))

    def copy(key, src, dst, device):
        at = number(key)
        return remote(src, dst, send_sem.at[at], recv_sem.at[at], device)

    def send(key, src, dst, device):
        order_of_sends.append((key, src, dst, device))
        copy(key, src, dst, device).start()

    def arrive(key, part):
        copy(key, part, part, partner).wait_recv()

    barrier = pltpu.get_barrier_semaphore()
    for device in (partner, across, beside, above, pair):
        pl.semaphore_signal(
            barrier, inc=1, device_id=device, device_id_type=pl.DeviceIdType.MESH
        )

    loads = []
    for index in range(layers):
        for p in range(2):
            loads.append((wq_hbm.at[index, :, pl.ds(p * columns, columns)], wq.at[index, p]))
        loads.append((wo_hbm.at[index], wo.at[index, 0]))

    def load(n):
        return pltpu.make_async_copy(loads[n][0], loads[n][1], load_sem.at[n])

    for n in range(len(loads)):
        load(n).start()

    def home(index, chunk):
        if chunk < 2:
            return wq_hbm.at[index, :, pl.ds(chunk * columns, columns)], wq.at[index, 4 + 2 * chunk]
        return wo_hbm.at[index], wo.at[index, 2]

    def extent(chunk):
        return width if chunk < 2 else depth

    def cut(index, chunk, kind):
        alone, shared = pieces(index, extent(chunk))
        cuts = 2 if chunk < 2 else 1
        size = alone if kind[0] == "a" else shared
        if not size:
            return []
        x_of = x_at if kind[1] == "s" else 1 - x_at
        if kind[0] == "a":
            base = x_of * alone
        else:
            z_of = z_at if kind[2] == "s" else 1 - z_at
            base = 2 * alone + (x_of * 2 + z_of) * shared
        size //= cuts
        return [pl.ds(pl.multiple_of(base + c * size, 16), size) for c in range(cuts)]

    kinds = ("qss", "qso", "qos", "qoo", "as", "ao")
    every = [(index, chunk) for index in range(layers) for chunk in range(3)]
    homes = {which: home(*which) for which in every}
    theres = {
        (index, chunk): wq.at[index, 5 + 2 * chunk] if chunk < 2 else wo.at[index, 3]
        for index, chunk in every
    }
    parts_of = {
        (*which, kind): [homes[which][1].at[at] for at in cut(*which, kind)]
        for which in every
        for kind in kinds
    }

    def first(index, chunk):
        source, _ = homes[index, chunk]
        for kind in ("qss", "as"):
            for c, at in enumerate(cut(index, chunk, kind)):
                part = parts_of[index, chunk, kind][c]
                send(("y", index, chunk, kind, c), source.at[at], part, across)

    def second(index, chunk):
        for c, part in enumerate(parts_of[index, chunk, "qss"]):
            arrive(("y", index, chunk, "qss", c), part)
            send(("x", index, chunk, "q", c), part, part, beside)
            send(("z", index, chunk, "s", c), part, part, above)

    def third(index, chunk):
        for c, part in enumerate(parts_of[index, chunk, "as"]):
            arrive(("y", index, chunk, "as", c), part)
            send(("x", index, chunk, "a", c), part, part, beside)

    def then(index, chunk):
        if index:
            third(index, chunk)
        for c, part in enumerate(parts_of[index, chunk, "qos"]):
            arrive(("x", index, chunk, "q", c), part)
            send(("z", index, chunk, "o", c), part, part, above)

    def fourth(index, chunk):
        for c, part in enumerate(parts_of[index, chunk, "ao"]):
            arrive(("x", index, chunk, "a", c), part)
        for c, part in enumerate(parts_of[index, chunk, "qso"]):
            arrive(("z", index, chunk, "s", c), part)
        for c, part in enumerate(parts_of[index, chunk, "qoo"]):
            arrive(("z", index, chunk, "o", c), part)
        if index or chunk == 2:
            send(("f", index, chunk), homes[index, chunk][1], theres[index, chunk], partner)

    def fifth(index, chunk):
        arrive(("f", index, chunk), theres[index, chunk])

    def share(index, chunk):
        source, _ = home(index, chunk)
        there = wq.at[index, 2 + chunk] if chunk < 2 else wo.at[index, 1]
        send(("w", index, chunk), source, there, partner)

    def shared(index, chunk):
        there = wq.at[index, 2 + chunk] if chunk < 2 else wo.at[index, 1]
        arrive(("w", index, chunk), there)

    def column_of(row):
        return jnp.transpose(jnp.broadcast_to(row.astype(f32), (LANES, row.shape[1])))

    half = rows // 2

    def normed(index, part):
        at = pl.ds(part * half, half)
        xs[index, 0, at, :] = layer_norm(
            stream[at, :].astype(f32), gain_ref[index : index + 1, :]
        )

    def exchange(index, part):
        at = pl.ds(part * half, half)
        send(
            ("n", index, part), xs.at[index, 0, at], xs.at[index, 1, at],
            pair if index else partner,
        )

    def exchanged(index, part):
        arrive(("n", index, part), xs.at[index, 1, pl.ds(part * half, half)])

    pl.semaphore_wait(barrier, 5)
    for chunk in range(3):
        first(0, chunk)
    column = column_of(order_ref[...])[:, :1]
    picks = (column == lax.broadcasted_iota(jnp.int32, (1, rows), 1).astype(f32)).astype(bf16)
    stream[...] = jnp.dot(picks, points_ref[...], preferred_element_type=f32).astype(bf16)
    normed(0, 0)
    normed(0, 1)
    spot = (lane % HEAD_DIM).astype(f32)

    def mark(side, row):
        own = column_of(row)
        tag_q[side] = jnp.where((spot < SCANS) & (own != spot), 1.0, 0.0)
        tag_k[side] = jnp.where(own == spot, BLOCKED, 0.0)

    mark(0, tag_ref[...])

    send(("t", 0), tag_ref, tags.at[0], partner)
    send(("t", 1), tag_ref, tags.at[1], pair)
    exchange(0, 0)
    exchange(0, 1)
    share(0, 2)
    for chunk in range(3):
        share(1, chunk)
    for chunk in range(3):
        first(1, chunk)

    def place(side, turn, left, right, middle):
        at = pl.ds(side * rows, rows)
        marks = tag_k[side]
        keys[turn, 0, at, :] = jnp.where(low, marks, left).astype(bf16)
        values[turn, 0, at, :] = jnp.where(low, middle, 1.0).astype(bf16)
        keys[turn, 1, at, :] = jnp.where(low, right, marks).astype(bf16)
        values[turn, 1, at, :] = jnp.where(low, 1.0, right).astype(bf16)

    def project(index, k, side, q_at, turn):
        result = jnp.dot(xs[index, side], wq[index, k], preferred_element_type=f32)
        left, middle, right = (result[:, LANES * n : LANES * (n + 1)] for n in range(3))
        place(side, turn, left, right, middle)
        marks = tag_q[side]
        query[q_at, 0] = jnp.where(
            low, marks, pltpu.roll(left * LOG2_SCALE, HEAD_DIM, 1)
        ).astype(bf16)
        query[q_at, 1] = jnp.where(
            low, pltpu.roll(middle * LOG2_SCALE, HEAD_DIM, 1), marks
        ).astype(bf16)

    def project_pair(k, turn):
        left, middle, right = (wq[1, k, :, LANES * n : LANES * (n + 1)] for n in range(3))
        weights = jnp.concatenate([jnp.where(low, middle, left), right], axis=1)
        result = jnp.dot(xs[1, 1], weights, preferred_element_type=f32)
        left, right = result[:, :LANES], result[:, LANES:]
        place(1, turn, left, right, left)

    def scores(q_at, turn, head, at, over):
        return lax.dot_general(
            query[q_at, head, at, :], keys[turn, head, over, :], (((1,), (1,)), ((), ())),
            preferred_element_type=f32,
        )

    def settle(target, k, at, sums):
        parts = [t / pltpu.roll(t, HEAD_DIM, 1) for t in sums]
        target[k, at, :] = jnp.where(low, parts[0], parts[1]).astype(bf16)

    row_blocks = [pl.ds(r * half, half) for r in range(2)]

    def flow(units, beside_first=None):
        table = units[0][0]()
        for n, (_, use) in enumerate(units):
            ahead = units[n + 1][0]() if n + 1 < len(units) else None
            if n == 0 and beside_first is not None:
                beside_first()
            use(table)
            table = ahead

    def attend(side, finish):
        units = []
        for at in row_blocks:
            sums = []
            for head in range(2):
                def look(head=head, at=at):
                    return scores(side, 0, head, at, slice(None))

                def use(table, head=head, at=at, sums=sums):
                    top = jnp.max(table, axis=-1, keepdims=True)
                    expo = jnp.exp2(table - top).astype(bf16)
                    sums.append(
                        jnp.dot(expo, values[0, head], preferred_element_type=f32)
                    )
                    if head == 1:
                        finish(at, sums)

                units.append((look, use))
        return units

    def attend_own(k, turn):
        over = pl.ds(0, rows)
        units = []
        for at in row_blocks:
            for head in range(2):
                def look(head=head, at=at):
                    return scores(k, turn, head, at, over)

                def use(table, head=head, at=at):
                    top = jnp.max(table, axis=-1, keepdims=True)
                    expo = jnp.exp2(table - top).astype(bf16)
                    acc[k, head, at, :] = jnp.dot(
                        expo, values[turn, head, over, :], preferred_element_type=f32
                    )
                    peak[k, head, at, :] = jnp.broadcast_to(top, (half, LANES))

                units.append((look, use))
        return units

    def attend_pair(k, turn):
        over = pl.ds(rows, rows)
        units = []
        for at in row_blocks:
            sums = []
            for head in range(2):
                def look(head=head, at=at):
                    return scores(k, turn, head, at, over)

                def use(table, head=head, at=at, sums=sums):
                    before = peak[k, head, at, :]
                    highest = jnp.max(table, axis=-1, keepdims=True)
                    top = jnp.maximum(before, jnp.broadcast_to(highest, (half, LANES)))
                    expo = jnp.concatenate(
                        [
                            jnp.exp2(table[:, LANES * n : LANES * (n + 1)] - top).astype(bf16)
                            for n in range(rows // LANES)
                        ],
                        axis=1,
                    )
                    sums.append(
                        jnp.dot(expo, values[turn, head, over, :], preferred_element_type=f32)
                        + acc[k, head, at, :] * jnp.exp2(before - top)
                    )
                    if head == 1:
                        settle(att, k, at, sums)

                units.append((look, use))
        return units

    def leave(index, part):
        at = pl.ds(part * half, half)
        result = stream[at, :].astype(f32)
        for slot, (one, two) in enumerate(((0, 1), (2, 3), (4, 6), (5, 7))):
            result += jnp.dot(
                jnp.concatenate([att[one, at, :], att[two, at, :]], axis=1),
                wo[index, slot],
                preferred_element_type=f32,
            )
        return result.astype(bf16)

    def run(count, events, *phases):
        def step(k, carry):
            for n, phase in enumerate(phases):
                for (when, place_in), todo in events.items():
                    if place_in == n:

                        @pl.when(k == when)
                        def _(todo=todo):
                            for event, args in todo:
                                event(*args)

                phase(k)
            return carry

        lax.fori_loop(0, count, step, 0)

    arrive(("t", 0), tags.at[0])
    mark(1, tags[0])
    exchanged(0, 0)
    exchanged(0, 1)

    def loaded(n):
        load(n).wait()

    def slot_of(k):
        return k + k // 2 * k

    def handed(k):
        to = 2 + k + k // 2 * (k - 1)
        return remote(given.at[k], att.at[to], given_send.at[k], given_recv.at[k], partner)

    def taken(k):
        to = 2 + k + k // 2 * (k - 1)
        part = att.at[to]
        return remote(part, part, given_send.at[k], given_recv.at[k], partner)

    def make(k):
        slot = slot_of(k)
        for side in range(2):
            project(0, slot, side, side, 0)

    def weigh(k):
        def give(at, sums):
            settle(given, k, at, sums)
            if at is row_blocks[-1]:
                handed(k).start()

        def keep(at, sums):
            settle(att, slot_of(k), at, sums)

        flow(attend(1, give) + attend(0, keep))

    run(
        4,
        {
            (0, 0): [(loaded, (0,)), (loaded, (1,))],
            (0, 1): [(second, (0, 0))],
            (1, 0): [(third, (0, 0)), (then, (0, 0))],
            (1, 1): [(second, (0, 1)), (third, (0, 1))],
            (2, 0): [(then, (0, 1)), (fourth, (0, 0))],
            (2, 1): [(second, (0, 2)), (third, (0, 2))],
            (3, 0): [(then, (0, 2)), (fourth, (0, 1)), (second, (1, 0))],
            (3, 1): [(fourth, (0, 2))],
        },
        make, weigh,
    )
    then(1, 0)
    second(1, 1)
    loaded(2)
    shared(0, 2)
    fifth(0, 2)
    for k in range(4):
        taken(k).wait_recv()
    for part in range(2):
        at = pl.ds(part * half, half)
        stream[at, :] = leave(0, part)
        normed(1, part)
        exchange(1, part)
    then(1, 1)
    second(1, 2)
    arrive(("t", 1), tags.at[1])
    mark(1, tags[1])

    loaded(3)
    loaded(4)
    project(1, 0, 0, 0, 0)

    def inner(k):
        flow(attend_own(k, k % 2), lambda: project(1, k + 1, 0, k + 1, (k + 1) % 2))

    run(
        steps - 1,
        {
            (1, 0): [(shared, (1, 0)), (fourth, (1, 0)), (then, (1, 2))],
            (2, 0): [(shared, (1, 1))],
            (3, 0): [],
            (4, 0): [(fifth, (1, 0)), (fourth, (1, 1))],
            (6, 0): [(fourth, (1, 2)), (fifth, (1, 1))],
        },
        inner,
    )
    flow(attend_own(steps - 1, 1))
    exchanged(1, 0)
    exchanged(1, 1)

    project_pair(0, 0)

    def outer(k):
        flow(attend_pair(k, k % 2), lambda: project_pair(k + 1, (k + 1) % 2))

    run(steps - 1, {}, outer)
    flow(attend_pair(steps - 1, 1))
    loaded(5)
    shared(1, 2)
    fifth(1, 2)
    for part in range(2):
        out_ref[pl.ds(part * half, half), :] = leave(1, part)

    for key, src, dst, device in order_of_sends:
        copy(key, src, dst, device).wait_send()
    for k in range(4):
        handed(k).wait_send()


def fused(points, order, scan_ids, ln_gain, w_qkv, w_out):
    rows, width = points.shape
    peers, ranges = lax.axis_size("head"), lax.axis_size("curve")
    layers, _, columns = w_qkv.shape
    columns //= 2
    steps = 2 * peers
    vmem, far = pl.BlockSpec(memory_space=pltpu.VMEM), pl.BlockSpec(memory_space=pl.ANY)
    dma = pltpu.SemaphoreType.DMA
    bf16, f32 = jnp.bfloat16, jnp.float32
    return pl.pallas_call(
        functools.partial(fused_kernel, peers, ranges),
        out_shape=jax.ShapeDtypeStruct((rows, width), bf16),
        in_specs=[vmem] * 4 + [far] * 2,
        out_specs=vmem,
        scratch_shapes=[
            pltpu.VMEM((layers, 2, rows, width), bf16),
            pltpu.VMEM((rows, width), bf16),
            pltpu.VMEM((layers, steps, width, columns), bf16),
            pltpu.VMEM((layers, peers, width // peers, width), bf16),
            pltpu.VMEM((steps, 2, rows, LANES), bf16),
            pltpu.VMEM((2, 2, 2 * rows, LANES), bf16),
            pltpu.VMEM((2, 2, 2 * rows, LANES), bf16),
            pltpu.VMEM((steps, rows, LANES), bf16),
            pltpu.VMEM((steps, 2, rows, LANES), f32),
            pltpu.VMEM((steps, 2, rows, LANES), f32),
            pltpu.VMEM((2, 1, rows), jnp.int32),
            pltpu.VMEM((2, rows, LANES), f32),
            pltpu.VMEM((2, rows, LANES), f32),
            pltpu.VMEM((steps // 2, rows, LANES), bf16),
            dma((96,)),
            dma((96,)),
            dma((3 * layers,)),
            dma((steps // 2,)),
            dma((steps // 2,)),
        ],
        compiler_params=pltpu.CompilerParams(
            collective_id=0, has_side_effects=True, vmem_limit_bytes=60 * 1024 * 1024
        ),
        cost_estimate=pl.CostEstimate(
            flops=80 * rows * width * width, bytes_accessed=20 * rows * width, transcendentals=0
        ),
    )(points, order, scan_ids.reshape(1, -1), ln_gain, w_qkv, w_out)


def chip_holds_window(points, w_qkv):
    peers, ranges = lax.axis_size("head"), lax.axis_size("curve")
    rows, width = points.shape
    return (
        peers == 4
        and ranges % 4 == 0
        and PATCH == 2 * rows
        and w_qkv.shape[0] == 2
        and w_qkv.shape[2] == 12 * HEAD_DIM
        and width == peers * 4 * HEAD_DIM
    )


def on_device(points, order, scan_ids, ln_gain, w_qkv, w_out):
    if chip_holds_window(points, w_qkv):
        return fused(points, order, scan_ids, ln_gain, w_qkv, w_out)
    stream = points[order[0]]
    tag_row = scan_ids.reshape(1, 1, -1)
    for index in range(2):
        normed = layer_norm(stream, ln_gain[index])
        stream = layer(index, stream, normed, tag_row, w_qkv[index], w_out[index])
    return stream


def solution(mesh):
    in_specs = (
        P(("curve", "head"), None),
        P(("curve", "head"), None),
        P(("curve", "head")),
        P(),
        P(None, None, "head"),
        P(None, "head", None),
    )
    out_specs = P(("curve", "head"), None)
    return jax.shard_map(
        on_device, mesh=mesh, in_specs=in_specs, out_specs=out_specs, check_vma=False
    )
```

```python
import functools

import jax
import jax.numpy as jnp
from jax import lax
from jax.experimental import pallas as pl
from jax.experimental.pallas import tpu as pltpu
from jax.sharding import PartitionSpec as P

HEAD_DIM = 64
PATCH = 1024


EPSILON = 1e-05


def layer_norm(rows, gain):
    values = rows.astype(jnp.float32)
    center = values - jnp.mean(values, axis=-1, keepdims=True)
    spread = jnp.mean(center * center, axis=-1, keepdims=True)
    return (center * lax.rsqrt(spread + EPSILON) * gain).astype(jnp.bfloat16)


def remote(src, dst, send_sem, recv_sem, device):
    return pltpu.make_async_remote_copy(
        src_ref=src,
        dst_ref=dst,
        send_sem=send_sem,
        recv_sem=recv_sem,
        device_id=device,
        device_id_type=pl.DeviceIdType.MESH,
    )


def layer_kernel(
    peers, ranges, halo, x_ref, tag_ref, w_ref, wo_ref, stream_ref, out_ref,
    all_x, q_buf, kv_buf, tags, att, heads, all_wo,
    x_recv, x_send, w_recv, w_send, t_recv, t_send, h_recv, h_send, kv_recv, kv_send,
):
    chunks, chunk_rows, _ = x_ref.shape
    rows = chunks * chunk_rows
    heads_local = w_ref.shape[1] // (3 * HEAD_DIM)
    chips = peers // 2
    window_blocks = PATCH // rows
    curve = lax.axis_index("curve")
    me = lax.axis_index("head")
    chip, core = me // 2, me % 2
    partner = chip * 2 + 1 - core
    up, down = {"curve": (curve + 1) % ranges}, {"curve": (curve + ranges - 1) % ranges}
    same = [((chip + s) % chips) * 2 + core for s in range(chips)]
    other = [((chip + s) % chips) * 2 + 1 - core for s in range(chips)]
    others = [(me + t) % peers for t in range(1, peers)]

    barrier = pltpu.get_barrier_semaphore()
    for blk in others:
        pl.semaphore_signal(
            barrier, inc=1, device_id={"head": blk}, device_id_type=pl.DeviceIdType.MESH
        )
    if halo:
        for neighbour in (up, down):
            pl.semaphore_signal(
                barrier, inc=1, device_id=neighbour, device_id_type=pl.DeviceIdType.MESH
            )
    pl.semaphore_wait(barrier, peers - 1 + (2 if halo else 0))

    def direct_x(s, c):
        dest = partner if s == 0 else same[s]
        return remote(
            x_ref.at[c], all_x.at[me, c], x_send.at[s, c], x_recv.at[me, c], {"head": dest}
        )

    def passed_x(s, c):
        part = all_x.at[same[s], c]
        return remote(
            part, part, x_send.at[chips + s, c], x_recv.at[same[s], c], {"head": partner}
        )

    def wait_x(blk, c):
        part = all_x.at[blk, c]
        remote(part, part, x_send.at[0, c], x_recv.at[blk, c], {"head": partner}).wait_recv()

    def tag_copy(t):
        return remote(
            tag_ref.at[0], tags.at[halo + me], t_send.at[t], t_recv.at[halo + me],
            {"head": others[t]},
        )

    def direct_w(s):
        dest = partner if s == 0 else same[s]
        return remote(wo_ref, all_wo.at[me], w_send.at[s], w_recv.at[me], {"head": dest})

    def passed_w(s):
        part = all_wo.at[same[s]]
        return remote(
            part, part, w_send.at[chips + s], w_recv.at[same[s]], {"head": partner}
        )

    def wait_w(blk):
        part = all_wo.at[blk]
        remote(part, part, w_send.at[0], w_recv.at[blk], {"head": partner}).wait_recv()

    def edge(buffer, send, recv, j):
        if j < halo:
            src, dst, device = buffer.at[peers + j], buffer.at[j], up
        else:
            src, dst, device = buffer.at[j], buffer.at[peers + j], down
        return remote(src, dst, send.at[j], recv.at[j], device)

    tag_send_edge = peers - 1

    for s in range(chips):
        for c in range(chunks):
            direct_x(s, c).start()
    for t in range(peers - 1):
        tag_copy(t).start()
    direct_w(0).start()
    tags[halo + me] = tag_ref[0]

    def project(values, blk, first_row):
        result = jnp.dot(values, w_ref[...], preferred_element_type=jnp.float32)
        result = result.astype(jnp.bfloat16)
        at = pl.ds(first_row, chunk_rows)
        for head in range(heads_local):
            base = head * 3 * HEAD_DIM
            q_buf[blk, at, head * HEAD_DIM : (head + 1) * HEAD_DIM] = result[
                :, base : base + HEAD_DIM
            ] * jnp.bfloat16(HEAD_DIM ** (-0.5))
            kv_buf[halo + blk, at, head * 2 * HEAD_DIM : (head + 1) * 2 * HEAD_DIM] = result[
                :, base + HEAD_DIM : base + 3 * HEAD_DIM
            ]

    def project_block(blk):
        for c in range(chunks):
            project(all_x[blk, c], blk, c * chunk_rows)

    def attend(blk):
        first = (blk + halo) // window_blocks * window_blocks
        column = jnp.transpose(
            jnp.broadcast_to(tags[halo + blk].astype(jnp.float32), (128, rows))
        )[:, :1]
        line = jnp.concatenate(
            [tags[first + j].astype(jnp.float32) for j in range(window_blocks)], axis=1
        )
        bias = jnp.where(column == line, 0.0, -jnp.inf)
        ones = jnp.ones((PATCH, HEAD_DIM), jnp.bfloat16)
        for head in range(heads_local):
            at = head * 2 * HEAD_DIM
            wide = kv_buf[pl.ds(first, window_blocks), :, at : at + 2 * HEAD_DIM].reshape(
                PATCH, 2 * HEAD_DIM
            )
            query = q_buf[blk, :, head * HEAD_DIM : (head + 1) * HEAD_DIM]
            scores = lax.dot_general(
                query, wide[:, :HEAD_DIM], (((1,), (1,)), ((), ())),
                preferred_element_type=jnp.float32,
            ) + bias
            row_max = jnp.max(scores, axis=-1, keepdims=True)
            expo = jnp.exp(scores - row_max).astype(jnp.bfloat16)
            result = jnp.dot(
                expo,
                jnp.concatenate([wide[:, HEAD_DIM:], ones], axis=1),
                preferred_element_type=jnp.float32,
            )
            normal = result[:, :HEAD_DIM] / result[:, HEAD_DIM : HEAD_DIM + 1]
            att[blk, :, head * HEAD_DIM : (head + 1) * HEAD_DIM] = normal.astype(jnp.bfloat16)

    def head_copy(t):
        blk = others[t]
        return remote(
            att.at[blk], heads.at[me], h_send.at[t], h_recv.at[me], {"head": blk}
        )

    def head_copy_to(blk):
        t = (blk - me + peers - 1) % peers
        return remote(
            att.at[blk], heads.at[me], h_send.at[t], h_recv.at[me], {"head": blk}
        )

    for c in range(chunks):
        project(x_ref[c], me, c * chunk_rows)
    for c in range(chunks):
        wait_x(partner, c)
    project_block(partner)
    for blk in others:
        part = tags.at[halo + blk]
        remote(part, part, t_send.at[0], t_recv.at[halo + blk], {"head": partner}).wait_recv()
    if halo:
        for j in range(2 * halo):
            edge(tags, t_send.at[pl.ds(peers, 2 * halo)], t_recv.at[pl.ds(peers + 2 * halo, 2 * halo)], j).start()

    early = not halo and window_blocks == 2
    if early:
        attend(me)
        attend(partner)
        head_copy_to(partner).start()
    for s in range(1, chips):
        for c in range(chunks):
            wait_x(same[s], c)
            passed_x(s, c).start()
            project(all_x[same[s], c], same[s], c * chunk_rows)
    for s in range(1, chips):
        direct_w(s).start()
        for c in range(chunks):
            wait_x(other[s], c)
            project(all_x[other[s], c], other[s], c * chunk_rows)
    if halo:
        for j in range(2 * halo):
            edge(kv_buf, kv_send, kv_recv, j).start()
        middle = chips // 2 if window_blocks == 2 else 0
        for j in range(2 * halo):
            edge(tags, t_send.at[pl.ds(peers, 2 * halo)], t_recv.at[pl.ds(peers + 2 * halo, 2 * halo)], j).wait_recv()

    def finish(blk):
        attend(blk)

        @pl.when(blk != me)
        def _():
            head_copy_to(blk).start()

    if early:
        for s in range(1, chips):
            finish(other[s])
            finish(same[s])
    else:
        if halo:
            inner = list(range(halo, peers - halo))
            outer = list(range(peers - halo, peers)) + list(range(halo))

            def inner_step(i, carry):
                finish(halo + (me + 1 + i) % (peers - 2 * halo))
                return carry

            lax.fori_loop(0, len(inner), inner_step, 0)
            for j in range(2 * halo):
                edge(kv_buf, kv_send, kv_recv, j).wait_recv()

            def outer_step(i, carry):
                finish((peers - halo + (me + i) % (2 * halo)) % peers)
                return carry

            lax.fori_loop(0, len(outer), outer_step, 0)
        else:

            def step(i, carry):
                finish((me + 1 + i) % peers)
                return carry

            lax.fori_loop(0, peers, step, 0)

    wait_w(partner)
    for s in range(1, chips):
        wait_w(same[s])
        passed_w(s).start()
    heads[me] = att[me]
    all_wo[me] = wo_ref[...]
    for s in range(1, chips):
        wait_w(other[s])
    for blk in others:
        part = heads.at[blk]
        remote(part, part, h_send.at[0], h_recv.at[blk], {"head": partner}).wait_recv()

    for c in range(chunks):
        at = pl.ds(c * chunk_rows, chunk_rows)
        total = stream_ref[at, :].astype(jnp.float32)
        for blk in range(peers):
            total += jnp.dot(
                heads[blk, at, :], all_wo[blk], preferred_element_type=jnp.float32
            )
        out_ref[at, :] = total.astype(jnp.bfloat16)

    for s in range(chips):
        for c in range(chunks):
            direct_x(s, c).wait_send()
            if s:
                passed_x(s, c).wait_send()
        direct_w(s).wait_send()
        if s:
            passed_w(s).wait_send()
    for t in range(peers - 1):
        tag_copy(t).wait_send()
        head_copy(t).wait_send()
    for j in range(2 * halo):
        edge(tags, t_send.at[pl.ds(peers, 2 * halo)], t_recv.at[pl.ds(peers + 2 * halo, 2 * halo)], j).wait_send()
        edge(kv_buf, kv_send, kv_recv, j).wait_send()


def layer(index, stream, normed, tag_row, weights, out_weights):
    rows, width = stream.shape
    peers, ranges = lax.axis_size("head"), lax.axis_size("curve")
    halo = PATCH // 2 // rows if index else 0
    chips = peers // 2
    chunks = max(1, rows // 256)
    columns = out_weights.shape[0]
    vmem = pl.BlockSpec(memory_space=pltpu.VMEM)
    dma = pltpu.SemaphoreType.DMA
    bf16 = jnp.bfloat16
    return pl.pallas_call(
        functools.partial(layer_kernel, peers, ranges, halo),
        out_shape=jax.ShapeDtypeStruct((rows, width), bf16),
        in_specs=[vmem] * 5,
        out_specs=vmem,
        scratch_shapes=[
            pltpu.VMEM((peers, chunks, rows // chunks, width), bf16),
            pltpu.VMEM((peers, rows, columns), bf16),
            pltpu.VMEM((peers + 2 * halo, rows, 2 * columns), bf16),
            pltpu.VMEM((peers + 2 * halo, 1, rows), jnp.int32),
            pltpu.VMEM((peers, rows, columns), bf16),
            pltpu.VMEM((peers, rows, columns), bf16),
            pltpu.VMEM((peers, columns, width), bf16),
            dma((peers, chunks)),
            dma((peers, chunks)),
            dma((peers,)),
            dma((peers,)),
            dma((peers + 4 * halo,)),
            dma((peers + 2 * halo,)),
            dma((peers,)),
            dma((peers,)),
            dma((max(1, 2 * halo),)),
            dma((max(1, 2 * halo),)),
        ],
        compiler_params=pltpu.CompilerParams(collective_id=index, has_side_effects=True),
        cost_estimate=pl.CostEstimate(
            flops=20 * rows * width * width, bytes_accessed=20 * rows * width, transcendentals=0
        ),
    )(
        normed.reshape(chunks, rows // chunks, width),
        tag_row,
        weights,
        out_weights,
        stream,
    )


SCANS = 4
BLOCKED = -1e30
LOG2_SCALE = 1.4426950408889634 * HEAD_DIM ** (-0.5)
LANES = 128


def pieces(index, extent):
    alone = extent // 8
    return alone, (extent - 2 * alone) // 4


def fused_kernel(
    peers, ranges,
    points_ref, order_ref, tag_ref, gain_ref, wq_hbm, wo_hbm, out_ref,
    xs, stream, wq, wo, query, keys, values, att, acc, peak, tags, tag_q, tag_k,
    given, send_sem, recv_sem, load_sem, given_send, given_recv,
):
    rows, width = points_ref.shape
    layers, steps, _, columns = wq.shape
    depth = wo_hbm.shape[1]
    curve = lax.axis_index("curve")
    me = lax.axis_index("head")
    chip, core = me // 2, me % 2
    x_at, z_at = curve % 2, curve // 2 % 2
    partner = {"head": chip * 2 + 1 - core}
    across = {"head": (me + 2) % peers}
    beside = {"curve": curve + 1 - 2 * x_at}
    above = {"curve": curve + 2 - 4 * z_at}
    total = peers * ranges
    block = (curve * peers + me + 2 * core - 1 + total) % total
    pair = {"curve": block // peers, "head": block % peers}

    bf16, f32 = jnp.bfloat16, jnp.float32
    lane = lax.broadcasted_iota(jnp.int32, (1, LANES), 1)
    low = lane < HEAD_DIM
    numbers, order_of_sends = {}, []

    def number(key):
        return numbers.setdefault(key, len(numbers))

    def copy(key, src, dst, device):
        at = number(key)
        return remote(src, dst, send_sem.at[at], recv_sem.at[at], device)

    def send(key, src, dst, device):
        order_of_sends.append((key, src, dst, device))
        copy(key, src, dst, device).start()

    def arrive(key, part):
        copy(key, part, part, partner).wait_recv()

    barrier = pltpu.get_barrier_semaphore()
    for device in (partner, across, beside, above, pair):
        pl.semaphore_signal(
            barrier, inc=1, device_id=device, device_id_type=pl.DeviceIdType.MESH
        )

    loads = []
    for index in range(layers):
        for p in range(2):
            loads.append((wq_hbm.at[index, :, pl.ds(p * columns, columns)], wq.at[index, p]))
        loads.append((wo_hbm.at[index], wo.at[index, 0]))

    def load(n):
        return pltpu.make_async_copy(loads[n][0], loads[n][1], load_sem.at[n])

    for n in range(len(loads)):
        load(n).start()

    def home(index, chunk):
        if chunk < 2:
            return wq_hbm.at[index, :, pl.ds(chunk * columns, columns)], wq.at[index, 4 + 2 * chunk]
        return wo_hbm.at[index], wo.at[index, 2]

    def extent(chunk):
        return width if chunk < 2 else depth

    def cut(index, chunk, kind):
        alone, shared = pieces(index, extent(chunk))
        cuts = 2 if chunk < 2 else 1
        size = alone if kind[0] == "a" else shared
        if not size:
            return []
        x_of = x_at if kind[1] == "s" else 1 - x_at
        if kind[0] == "a":
            base = x_of * alone
        else:
            z_of = z_at if kind[2] == "s" else 1 - z_at
            base = 2 * alone + (x_of * 2 + z_of) * shared
        size //= cuts
        return [pl.ds(pl.multiple_of(base + c * size, 16), size) for c in range(cuts)]

    kinds = ("qss", "qso", "qos", "qoo", "as", "ao")
    every = [(index, chunk) for index in range(layers) for chunk in range(3)]
    homes = {which: home(*which) for which in every}
    theres = {
        (index, chunk): wq.at[index, 5 + 2 * chunk] if chunk < 2 else wo.at[index, 3]
        for index, chunk in every
    }
    parts_of = {
        (*which, kind): [homes[which][1].at[at] for at in cut(*which, kind)]
        for which in every
        for kind in kinds
    }

    def first(index, chunk):
        source, _ = homes[index, chunk]
        for kind in ("qss", "as"):
            for c, at in enumerate(cut(index, chunk, kind)):
                part = parts_of[index, chunk, kind][c]
                send(("y", index, chunk, kind, c), source.at[at], part, across)

    def second(index, chunk):
        for c, part in enumerate(parts_of[index, chunk, "qss"]):
            arrive(("y", index, chunk, "qss", c), part)
            send(("x", index, chunk, "q", c), part, part, beside)
            send(("z", index, chunk, "s", c), part, part, above)

    def third(index, chunk):
        for c, part in enumerate(parts_of[index, chunk, "as"]):
            arrive(("y", index, chunk, "as", c), part)
            send(("x", index, chunk, "a", c), part, part, beside)

    def then(index, chunk):
        if index:
            third(index, chunk)
        for c, part in enumerate(parts_of[index, chunk, "qos"]):
            arrive(("x", index, chunk, "q", c), part)
            send(("z", index, chunk, "o", c), part, part, above)

    def fourth(index, chunk):
        for c, part in enumerate(parts_of[index, chunk, "ao"]):
            arrive(("x", index, chunk, "a", c), part)
        for c, part in enumerate(parts_of[index, chunk, "qso"]):
            arrive(("z", index, chunk, "s", c), part)
        for c, part in enumerate(parts_of[index, chunk, "qoo"]):
            arrive(("z", index, chunk, "o", c), part)
        if index or chunk == 2:
            send(("f", index, chunk), homes[index, chunk][1], theres[index, chunk], partner)

    def fifth(index, chunk):
        arrive(("f", index, chunk), theres[index, chunk])

    def share(index, chunk):
        source, _ = home(index, chunk)
        there = wq.at[index, 2 + chunk] if chunk < 2 else wo.at[index, 1]
        send(("w", index, chunk), source, there, partner)

    def shared(index, chunk):
        there = wq.at[index, 2 + chunk] if chunk < 2 else wo.at[index, 1]
        arrive(("w", index, chunk), there)

    def column_of(row):
        return jnp.transpose(jnp.broadcast_to(row.astype(f32), (LANES, row.shape[1])))

    half = rows // 2

    def normed(index, part):
        at = pl.ds(part * half, half)
        xs[index, 0, at, :] = layer_norm(
            stream[at, :].astype(f32), gain_ref[index : index + 1, :]
        )

    def exchange(index, part):
        at = pl.ds(part * half, half)
        send(
            ("n", index, part), xs.at[index, 0, at], xs.at[index, 1, at],
            pair if index else partner,
        )

    def exchanged(index, part):
        arrive(("n", index, part), xs.at[index, 1, pl.ds(part * half, half)])

    pl.semaphore_wait(barrier, 5)
    for chunk in range(3):
        first(0, chunk)
    column = column_of(order_ref[...])[:, :1]
    picks = (column == lax.broadcasted_iota(jnp.int32, (1, rows), 1).astype(f32)).astype(bf16)
    stream[...] = jnp.dot(picks, points_ref[...], preferred_element_type=f32).astype(bf16)
    normed(0, 0)
    normed(0, 1)
    spot = (lane % HEAD_DIM).astype(f32)

    def mark(side, row):
        own = column_of(row)
        tag_q[side] = jnp.where((spot < SCANS) & (own != spot), 1.0, 0.0)
        tag_k[side] = jnp.where(own == spot, BLOCKED, 0.0)

    mark(0, tag_ref[...])

    send(("t", 0), tag_ref, tags.at[0], partner)
    send(("t", 1), tag_ref, tags.at[1], pair)
    exchange(0, 0)
    exchange(0, 1)
    share(0, 2)
    for chunk in range(3):
        share(1, chunk)
    for chunk in range(3):
        first(1, chunk)

    def place(side, turn, left, right, middle):
        at = pl.ds(side * rows, rows)
        marks = tag_k[side]
        keys[turn, 0, at, :] = jnp.where(low, marks, left).astype(bf16)
        values[turn, 0, at, :] = jnp.where(low, middle, 1.0).astype(bf16)
        keys[turn, 1, at, :] = jnp.where(low, right, marks).astype(bf16)
        values[turn, 1, at, :] = jnp.where(low, 1.0, right).astype(bf16)

    def project(index, k, side, q_at, turn):
        result = jnp.dot(xs[index, side], wq[index, k], preferred_element_type=f32)
        left, middle, right = (result[:, LANES * n : LANES * (n + 1)] for n in range(3))
        place(side, turn, left, right, middle)
        marks = tag_q[side]
        query[q_at, 0] = jnp.where(
            low, marks, pltpu.roll(left * LOG2_SCALE, HEAD_DIM, 1)
        ).astype(bf16)
        query[q_at, 1] = jnp.where(
            low, pltpu.roll(middle * LOG2_SCALE, HEAD_DIM, 1), marks
        ).astype(bf16)

    def project_pair(k, turn):
        left, middle, right = (wq[1, k, :, LANES * n : LANES * (n + 1)] for n in range(3))
        weights = jnp.concatenate([jnp.where(low, middle, left), right], axis=1)
        result = jnp.dot(xs[1, 1], weights, preferred_element_type=f32)
        left, right = result[:, :LANES], result[:, LANES:]
        place(1, turn, left, right, left)

    def scores(q_at, turn, head, at, over):
        return lax.dot_general(
            query[q_at, head, at, :], keys[turn, head, over, :], (((1,), (1,)), ((), ())),
            preferred_element_type=f32,
        )

    def settle(target, k, at, sums):
        parts = [t / pltpu.roll(t, HEAD_DIM, 1) for t in sums]
        target[k, at, :] = jnp.where(low, parts[0], parts[1]).astype(bf16)

    row_blocks = [pl.ds(r * half, half) for r in range(2)]

    def flow(units, beside_first=None):
        table = units[0][0]()
        for n, (_, use) in enumerate(units):
            ahead = units[n + 1][0]() if n + 1 < len(units) else None
            if n == 0 and beside_first is not None:
                beside_first()
            use(table)
            table = ahead

    def attend(side, finish):
        units = []
        for at in row_blocks:
            sums = []
            for head in range(2):
                def look(head=head, at=at):
                    return scores(side, 0, head, at, slice(None))

                def use(table, head=head, at=at, sums=sums):
                    top = jnp.max(table, axis=-1, keepdims=True)
                    expo = jnp.exp2(table - top).astype(bf16)
                    sums.append(
                        jnp.dot(expo, values[0, head], preferred_element_type=f32)
                    )
                    if head == 1:
                        finish(at, sums)

                units.append((look, use))
        return units

    def attend_own(k, turn):
        over = pl.ds(0, rows)
        units = []
        for at in row_blocks:
            for head in range(2):
                def look(head=head, at=at):
                    return scores(k, turn, head, at, over)

                def use(table, head=head, at=at):
                    top = jnp.max(table, axis=-1, keepdims=True)
                    expo = jnp.exp2(table - top).astype(bf16)
                    acc[k, head, at, :] = jnp.dot(
                        expo, values[turn, head, over, :], preferred_element_type=f32
                    )
                    peak[k, head, at, :] = jnp.broadcast_to(top, (half, LANES))

                units.append((look, use))
        return units

    def attend_pair(k, turn):
        over = pl.ds(rows, rows)
        units = []
        for at in row_blocks:
            sums = []
            for head in range(2):
                def look(head=head, at=at):
                    return scores(k, turn, head, at, over)

                def use(table, head=head, at=at, sums=sums):
                    before = peak[k, head, at, :]
                    highest = jnp.max(table, axis=-1, keepdims=True)
                    top = jnp.maximum(before, jnp.broadcast_to(highest, (half, LANES)))
                    expo = jnp.concatenate(
                        [
                            jnp.exp2(table[:, LANES * n : LANES * (n + 1)] - top).astype(bf16)
                            for n in range(rows // LANES)
                        ],
                        axis=1,
                    )
                    sums.append(
                        jnp.dot(expo, values[turn, head, over, :], preferred_element_type=f32)
                        + acc[k, head, at, :] * jnp.exp2(before - top)
                    )
                    if head == 1:
                        settle(att, k, at, sums)

                units.append((look, use))
        return units

    def leave(index, part):
        at = pl.ds(part * half, half)
        result = stream[at, :].astype(f32)
        for slot, (one, two) in enumerate(((0, 1), (2, 3), (4, 6), (5, 7))):
            result += jnp.dot(
                jnp.concatenate([att[one, at, :], att[two, at, :]], axis=1),
                wo[index, slot],
                preferred_element_type=f32,
            )
        return result.astype(bf16)

    def run(count, events, *phases):
        def step(k, carry):
            for n, phase in enumerate(phases):
                for (when, place_in), todo in events.items():
                    if place_in == n:

                        @pl.when(k == when)
                        def _(todo=todo):
                            for event, args in todo:
                                event(*args)

                phase(k)
            return carry

        lax.fori_loop(0, count, step, 0)

    arrive(("t", 0), tags.at[0])
    mark(1, tags[0])
    exchanged(0, 0)
    exchanged(0, 1)

    def loaded(n):
        load(n).wait()

    def slot_of(k):
        return k + k // 2 * k

    def handed(k):
        to = 2 + k + k // 2 * (k - 1)
        return remote(given.at[k], att.at[to], given_send.at[k], given_recv.at[k], partner)

    def taken(k):
        to = 2 + k + k // 2 * (k - 1)
        part = att.at[to]
        return remote(part, part, given_send.at[k], given_recv.at[k], partner)

    def make(k):
        slot = slot_of(k)
        for side in range(2):
            project(0, slot, side, side, 0)

    def weigh(k):
        def give(at, sums):
            settle(given, k, at, sums)
            if at is row_blocks[-1]:
                handed(k).start()

        def keep(at, sums):
            settle(att, slot_of(k), at, sums)

        flow(attend(1, give) + attend(0, keep))

    run(
        4,
        {
            (0, 0): [(loaded, (0,)), (loaded, (1,))],
            (0, 1): [(second, (0, 0))],
            (1, 0): [(third, (0, 0)), (then, (0, 0))],
            (1, 1): [(second, (0, 1)), (third, (0, 1))],
            (2, 0): [(then, (0, 1)), (fourth, (0, 0))],
            (2, 1): [(second, (0, 2)), (third, (0, 2))],
            (3, 0): [(then, (0, 2)), (fourth, (0, 1)), (second, (1, 0))],
            (3, 1): [(fourth, (0, 2))],
        },
        make, weigh,
    )
    then(1, 0)
    second(1, 1)
    loaded(2)
    shared(0, 2)
    fifth(0, 2)
    for k in range(4):
        taken(k).wait_recv()
    for part in range(2):
        at = pl.ds(part * half, half)
        stream[at, :] = leave(0, part)
        normed(1, part)
        exchange(1, part)
    then(1, 1)
    second(1, 2)
    arrive(("t", 1), tags.at[1])
    mark(1, tags[1])

    loaded(3)
    loaded(4)
    project(1, 0, 0, 0, 0)

    def inner(k):
        flow(attend_own(k, k % 2), lambda: project(1, k + 1, 0, k + 1, (k + 1) % 2))

    run(
        steps - 1,
        {
            (1, 0): [(shared, (1, 0)), (fourth, (1, 0))],
            (2, 0): [(shared, (1, 1))],
            (3, 0): [],
            (4, 0): [(fifth, (1, 0)), (fourth, (1, 1))],
            (6, 0): [(then, (1, 2)), (fifth, (1, 1))],
        },
        inner,
    )
    flow(attend_own(steps - 1, 1))
    exchanged(1, 0)
    exchanged(1, 1)
    fourth(1, 2)

    project_pair(0, 0)

    def outer(k):
        flow(attend_pair(k, k % 2), lambda: project_pair(k + 1, (k + 1) % 2))

    run(steps - 1, {}, outer)
    flow(attend_pair(steps - 1, 1))
    loaded(5)
    shared(1, 2)
    fifth(1, 2)
    for part in range(2):
        out_ref[pl.ds(part * half, half), :] = leave(1, part)

    for key, src, dst, device in order_of_sends:
        copy(key, src, dst, device).wait_send()
    for k in range(4):
        handed(k).wait_send()


def fused(points, order, scan_ids, ln_gain, w_qkv, w_out):
    rows, width = points.shape
    peers, ranges = lax.axis_size("head"), lax.axis_size("curve")
    layers, _, columns = w_qkv.shape
    columns //= 2
    steps = 2 * peers
    vmem, far = pl.BlockSpec(memory_space=pltpu.VMEM), pl.BlockSpec(memory_space=pl.ANY)
    dma = pltpu.SemaphoreType.DMA
    bf16, f32 = jnp.bfloat16, jnp.float32
    return pl.pallas_call(
        functools.partial(fused_kernel, peers, ranges),
        out_shape=jax.ShapeDtypeStruct((rows, width), bf16),
        in_specs=[vmem] * 4 + [far] * 2,
        out_specs=vmem,
        scratch_shapes=[
            pltpu.VMEM((layers, 2, rows, width), bf16),
            pltpu.VMEM((rows, width), bf16),
            pltpu.VMEM((layers, steps, width, columns), bf16),
            pltpu.VMEM((layers, peers, width // peers, width), bf16),
            pltpu.VMEM((steps, 2, rows, LANES), bf16),
            pltpu.VMEM((2, 2, 2 * rows, LANES), bf16),
            pltpu.VMEM((2, 2, 2 * rows, LANES), bf16),
            pltpu.VMEM((steps, rows, LANES), bf16),
            pltpu.VMEM((steps, 2, rows, LANES), f32),
            pltpu.VMEM((steps, 2, rows, LANES), f32),
            pltpu.VMEM((2, 1, rows), jnp.int32),
            pltpu.VMEM((2, rows, LANES), f32),
            pltpu.VMEM((2, rows, LANES), f32),
            pltpu.VMEM((steps // 2, rows, LANES), bf16),
            dma((96,)),
            dma((96,)),
            dma((3 * layers,)),
            dma((steps // 2,)),
            dma((steps // 2,)),
        ],
        compiler_params=pltpu.CompilerParams(
            collective_id=0, has_side_effects=True, vmem_limit_bytes=60 * 1024 * 1024
        ),
        cost_estimate=pl.CostEstimate(
            flops=80 * rows * width * width, bytes_accessed=20 * rows * width, transcendentals=0
        ),
    )(points, order, scan_ids.reshape(1, -1), ln_gain, w_qkv, w_out)


def chip_holds_window(points, w_qkv):
    peers, ranges = lax.axis_size("head"), lax.axis_size("curve")
    rows, width = points.shape
    return (
        peers == 4
        and ranges % 4 == 0
        and PATCH == 2 * rows
        and w_qkv.shape[0] == 2
        and w_qkv.shape[2] == 12 * HEAD_DIM
        and width == peers * 4 * HEAD_DIM
    )


def on_device(points, order, scan_ids, ln_gain, w_qkv, w_out):
    if chip_holds_window(points, w_qkv):
        return fused(points, order, scan_ids, ln_gain, w_qkv, w_out)
    stream = points[order[0]]
    tag_row = scan_ids.reshape(1, 1, -1)
    for index in range(2):
        normed = layer_norm(stream, ln_gain[index])
        stream = layer(index, stream, normed, tag_row, w_qkv[index], w_out[index])
    return stream


def solution(mesh):
    in_specs = (
        P(("curve", "head"), None),
        P(("curve", "head"), None),
        P(("curve", "head")),
        P(),
        P(None, None, "head"),
        P(None, "head", None),
    )
    out_specs = P(("curve", "head"), None)
    return jax.shard_map(
        on_device, mesh=mesh, in_specs=in_specs, out_specs=out_specs, check_vma=False
    )
```

```python
import functools

import jax
import jax.numpy as jnp
from jax import lax
from jax.experimental import pallas as pl
from jax.experimental.pallas import tpu as pltpu
from jax.sharding import PartitionSpec as P

HEAD_DIM = 64
PATCH = 1024


EPSILON = 1e-05


def layer_norm(rows, gain):
    values = rows.astype(jnp.float32)
    center = values - jnp.mean(values, axis=-1, keepdims=True)
    spread = jnp.mean(center * center, axis=-1, keepdims=True)
    return (center * lax.rsqrt(spread + EPSILON) * gain).astype(jnp.bfloat16)


def remote(src, dst, send_sem, recv_sem, device):
    return pltpu.make_async_remote_copy(
        src_ref=src,
        dst_ref=dst,
        send_sem=send_sem,
        recv_sem=recv_sem,
        device_id=device,
        device_id_type=pl.DeviceIdType.MESH,
    )


def layer_kernel(
    peers, ranges, halo, x_ref, tag_ref, w_ref, wo_ref, stream_ref, out_ref,
    all_x, q_buf, kv_buf, tags, att, heads, all_wo,
    x_recv, x_send, w_recv, w_send, t_recv, t_send, h_recv, h_send, kv_recv, kv_send,
):
    chunks, chunk_rows, _ = x_ref.shape
    rows = chunks * chunk_rows
    heads_local = w_ref.shape[1] // (3 * HEAD_DIM)
    chips = peers // 2
    window_blocks = PATCH // rows
    curve = lax.axis_index("curve")
    me = lax.axis_index("head")
    chip, core = me // 2, me % 2
    partner = chip * 2 + 1 - core
    up, down = {"curve": (curve + 1) % ranges}, {"curve": (curve + ranges - 1) % ranges}
    same = [((chip + s) % chips) * 2 + core for s in range(chips)]
    other = [((chip + s) % chips) * 2 + 1 - core for s in range(chips)]
    others = [(me + t) % peers for t in range(1, peers)]

    barrier = pltpu.get_barrier_semaphore()
    for blk in others:
        pl.semaphore_signal(
            barrier, inc=1, device_id={"head": blk}, device_id_type=pl.DeviceIdType.MESH
        )
    if halo:
        for neighbour in (up, down):
            pl.semaphore_signal(
                barrier, inc=1, device_id=neighbour, device_id_type=pl.DeviceIdType.MESH
            )
    pl.semaphore_wait(barrier, peers - 1 + (2 if halo else 0))

    def direct_x(s, c):
        dest = partner if s == 0 else same[s]
        return remote(
            x_ref.at[c], all_x.at[me, c], x_send.at[s, c], x_recv.at[me, c], {"head": dest}
        )

    def passed_x(s, c):
        part = all_x.at[same[s], c]
        return remote(
            part, part, x_send.at[chips + s, c], x_recv.at[same[s], c], {"head": partner}
        )

    def wait_x(blk, c):
        part = all_x.at[blk, c]
        remote(part, part, x_send.at[0, c], x_recv.at[blk, c], {"head": partner}).wait_recv()

    def tag_copy(t):
        return remote(
            tag_ref.at[0], tags.at[halo + me], t_send.at[t], t_recv.at[halo + me],
            {"head": others[t]},
        )

    def direct_w(s):
        dest = partner if s == 0 else same[s]
        return remote(wo_ref, all_wo.at[me], w_send.at[s], w_recv.at[me], {"head": dest})

    def passed_w(s):
        part = all_wo.at[same[s]]
        return remote(
            part, part, w_send.at[chips + s], w_recv.at[same[s]], {"head": partner}
        )

    def wait_w(blk):
        part = all_wo.at[blk]
        remote(part, part, w_send.at[0], w_recv.at[blk], {"head": partner}).wait_recv()

    def edge(buffer, send, recv, j):
        if j < halo:
            src, dst, device = buffer.at[peers + j], buffer.at[j], up
        else:
            src, dst, device = buffer.at[j], buffer.at[peers + j], down
        return remote(src, dst, send.at[j], recv.at[j], device)

    tag_send_edge = peers - 1

    for s in range(chips):
        for c in range(chunks):
            direct_x(s, c).start()
    for t in range(peers - 1):
        tag_copy(t).start()
    direct_w(0).start()
    tags[halo + me] = tag_ref[0]

    def project(values, blk, first_row):
        result = jnp.dot(values, w_ref[...], preferred_element_type=jnp.float32)
        result = result.astype(jnp.bfloat16)
        at = pl.ds(first_row, chunk_rows)
        for head in range(heads_local):
            base = head * 3 * HEAD_DIM
            q_buf[blk, at, head * HEAD_DIM : (head + 1) * HEAD_DIM] = result[
                :, base : base + HEAD_DIM
            ] * jnp.bfloat16(HEAD_DIM ** (-0.5))
            kv_buf[halo + blk, at, head * 2 * HEAD_DIM : (head + 1) * 2 * HEAD_DIM] = result[
                :, base + HEAD_DIM : base + 3 * HEAD_DIM
            ]

    def project_block(blk):
        for c in range(chunks):
            project(all_x[blk, c], blk, c * chunk_rows)

    def attend(blk):
        first = (blk + halo) // window_blocks * window_blocks
        column = jnp.transpose(
            jnp.broadcast_to(tags[halo + blk].astype(jnp.float32), (128, rows))
        )[:, :1]
        line = jnp.concatenate(
            [tags[first + j].astype(jnp.float32) for j in range(window_blocks)], axis=1
        )
        bias = jnp.where(column == line, 0.0, -jnp.inf)
        ones = jnp.ones((PATCH, HEAD_DIM), jnp.bfloat16)
        for head in range(heads_local):
            at = head * 2 * HEAD_DIM
            wide = kv_buf[pl.ds(first, window_blocks), :, at : at + 2 * HEAD_DIM].reshape(
                PATCH, 2 * HEAD_DIM
            )
            query = q_buf[blk, :, head * HEAD_DIM : (head + 1) * HEAD_DIM]
            scores = lax.dot_general(
                query, wide[:, :HEAD_DIM], (((1,), (1,)), ((), ())),
                preferred_element_type=jnp.float32,
            ) + bias
            row_max = jnp.max(scores, axis=-1, keepdims=True)
            expo = jnp.exp(scores - row_max).astype(jnp.bfloat16)
            result = jnp.dot(
                expo,
                jnp.concatenate([wide[:, HEAD_DIM:], ones], axis=1),
                preferred_element_type=jnp.float32,
            )
            normal = result[:, :HEAD_DIM] / result[:, HEAD_DIM : HEAD_DIM + 1]
            att[blk, :, head * HEAD_DIM : (head + 1) * HEAD_DIM] = normal.astype(jnp.bfloat16)

    def head_copy(t):
        blk = others[t]
        return remote(
            att.at[blk], heads.at[me], h_send.at[t], h_recv.at[me], {"head": blk}
        )

    def head_copy_to(blk):
        t = (blk - me + peers - 1) % peers
        return remote(
            att.at[blk], heads.at[me], h_send.at[t], h_recv.at[me], {"head": blk}
        )

    for c in range(chunks):
        project(x_ref[c], me, c * chunk_rows)
    for c in range(chunks):
        wait_x(partner, c)
    project_block(partner)
    for blk in others:
        part = tags.at[halo + blk]
        remote(part, part, t_send.at[0], t_recv.at[halo + blk], {"head": partner}).wait_recv()
    if halo:
        for j in range(2 * halo):
            edge(tags, t_send.at[pl.ds(peers, 2 * halo)], t_recv.at[pl.ds(peers + 2 * halo, 2 * halo)], j).start()

    early = not halo and window_blocks == 2
    if early:
        attend(me)
        attend(partner)
        head_copy_to(partner).start()
    for s in range(1, chips):
        for c in range(chunks):
            wait_x(same[s], c)
            passed_x(s, c).start()
            project(all_x[same[s], c], same[s], c * chunk_rows)
    for s in range(1, chips):
        direct_w(s).start()
        for c in range(chunks):
            wait_x(other[s], c)
            project(all_x[other[s], c], other[s], c * chunk_rows)
    if halo:
        for j in range(2 * halo):
            edge(kv_buf, kv_send, kv_recv, j).start()
        middle = chips // 2 if window_blocks == 2 else 0
        for j in range(2 * halo):
            edge(tags, t_send.at[pl.ds(peers, 2 * halo)], t_recv.at[pl.ds(peers + 2 * halo, 2 * halo)], j).wait_recv()

    def finish(blk):
        attend(blk)

        @pl.when(blk != me)
        def _():
            head_copy_to(blk).start()

    if early:
        for s in range(1, chips):
            finish(other[s])
            finish(same[s])
    else:
        if halo:
            inner = list(range(halo, peers - halo))
            outer = list(range(peers - halo, peers)) + list(range(halo))

            def inner_step(i, carry):
                finish(halo + (me + 1 + i) % (peers - 2 * halo))
                return carry

            lax.fori_loop(0, len(inner), inner_step, 0)
            for j in range(2 * halo):
                edge(kv_buf, kv_send, kv_recv, j).wait_recv()

            def outer_step(i, carry):
                finish((peers - halo + (me + i) % (2 * halo)) % peers)
                return carry

            lax.fori_loop(0, len(outer), outer_step, 0)
        else:

            def step(i, carry):
                finish((me + 1 + i) % peers)
                return carry

            lax.fori_loop(0, peers, step, 0)

    wait_w(partner)
    for s in range(1, chips):
        wait_w(same[s])
        passed_w(s).start()
    heads[me] = att[me]
    all_wo[me] = wo_ref[...]
    for s in range(1, chips):
        wait_w(other[s])
    for blk in others:
        part = heads.at[blk]
        remote(part, part, h_send.at[0], h_recv.at[blk], {"head": partner}).wait_recv()

    for c in range(chunks):
        at = pl.ds(c * chunk_rows, chunk_rows)
        total = stream_ref[at, :].astype(jnp.float32)
        for blk in range(peers):
            total += jnp.dot(
                heads[blk, at, :], all_wo[blk], preferred_element_type=jnp.float32
            )
        out_ref[at, :] = total.astype(jnp.bfloat16)

    for s in range(chips):
        for c in range(chunks):
            direct_x(s, c).wait_send()
            if s:
                passed_x(s, c).wait_send()
        direct_w(s).wait_send()
        if s:
            passed_w(s).wait_send()
    for t in range(peers - 1):
        tag_copy(t).wait_send()
        head_copy(t).wait_send()
    for j in range(2 * halo):
        edge(tags, t_send.at[pl.ds(peers, 2 * halo)], t_recv.at[pl.ds(peers + 2 * halo, 2 * halo)], j).wait_send()
        edge(kv_buf, kv_send, kv_recv, j).wait_send()


def layer(index, stream, normed, tag_row, weights, out_weights):
    rows, width = stream.shape
    peers, ranges = lax.axis_size("head"), lax.axis_size("curve")
    halo = PATCH // 2 // rows if index else 0
    chips = peers // 2
    chunks = max(1, rows // 256)
    columns = out_weights.shape[0]
    vmem = pl.BlockSpec(memory_space=pltpu.VMEM)
    dma = pltpu.SemaphoreType.DMA
    bf16 = jnp.bfloat16
    return pl.pallas_call(
        functools.partial(layer_kernel, peers, ranges, halo),
        out_shape=jax.ShapeDtypeStruct((rows, width), bf16),
        in_specs=[vmem] * 5,
        out_specs=vmem,
        scratch_shapes=[
            pltpu.VMEM((peers, chunks, rows // chunks, width), bf16),
            pltpu.VMEM((peers, rows, columns), bf16),
            pltpu.VMEM((peers + 2 * halo, rows, 2 * columns), bf16),
            pltpu.VMEM((peers + 2 * halo, 1, rows), jnp.int32),
            pltpu.VMEM((peers, rows, columns), bf16),
            pltpu.VMEM((peers, rows, columns), bf16),
            pltpu.VMEM((peers, columns, width), bf16),
            dma((peers, chunks)),
            dma((peers, chunks)),
            dma((peers,)),
            dma((peers,)),
            dma((peers + 4 * halo,)),
            dma((peers + 2 * halo,)),
            dma((peers,)),
            dma((peers,)),
            dma((max(1, 2 * halo),)),
            dma((max(1, 2 * halo),)),
        ],
        compiler_params=pltpu.CompilerParams(collective_id=index, has_side_effects=True),
        cost_estimate=pl.CostEstimate(
            flops=20 * rows * width * width, bytes_accessed=20 * rows * width, transcendentals=0
        ),
    )(
        normed.reshape(chunks, rows // chunks, width),
        tag_row,
        weights,
        out_weights,
        stream,
    )


SCANS = 4
BLOCKED = -1e30
LOG2_SCALE = 1.4426950408889634 * HEAD_DIM ** (-0.5)
LANES = 128


def pieces(index, extent):
    alone = extent // 8
    return alone, (extent - 2 * alone) // 4


def fused_kernel(
    peers, ranges,
    points_ref, order_ref, tag_ref, gain_ref, wq_hbm, wo_hbm, out_ref,
    xs, stream, wq, wo, query, keys, values, att, acc, peak, tags, tag_q, tag_k,
    given, send_sem, recv_sem, load_sem, given_send, given_recv,
):
    rows, width = points_ref.shape
    layers, steps, _, columns = wq.shape
    depth = wo_hbm.shape[1]
    curve = lax.axis_index("curve")
    me = lax.axis_index("head")
    chip, core = me // 2, me % 2
    x_at, z_at = curve % 2, curve // 2 % 2
    partner = {"head": chip * 2 + 1 - core}
    across = {"head": (me + 2) % peers}
    beside = {"curve": curve + 1 - 2 * x_at}
    above = {"curve": curve + 2 - 4 * z_at}
    total = peers * ranges
    block = (curve * peers + me + 2 * core - 1 + total) % total
    pair = {"curve": block // peers, "head": block % peers}

    bf16, f32 = jnp.bfloat16, jnp.float32
    lane = lax.broadcasted_iota(jnp.int32, (1, LANES), 1)
    low = lane < HEAD_DIM
    numbers, order_of_sends = {}, []

    def number(key):
        return numbers.setdefault(key, len(numbers))

    def copy(key, src, dst, device):
        at = number(key)
        return remote(src, dst, send_sem.at[at], recv_sem.at[at], device)

    def send(key, src, dst, device):
        order_of_sends.append((key, src, dst, device))
        copy(key, src, dst, device).start()

    def arrive(key, part):
        copy(key, part, part, partner).wait_recv()

    barrier = pltpu.get_barrier_semaphore()
    for device in (partner, across, beside, above, pair):
        pl.semaphore_signal(
            barrier, inc=1, device_id=device, device_id_type=pl.DeviceIdType.MESH
        )

    loads = []
    for index in range(layers):
        for p in range(2):
            loads.append((wq_hbm.at[index, :, pl.ds(p * columns, columns)], wq.at[index, p]))
        loads.append((wo_hbm.at[index], wo.at[index, 0]))

    def load(n):
        return pltpu.make_async_copy(loads[n][0], loads[n][1], load_sem.at[n])

    for n in range(len(loads)):
        load(n).start()

    def home(index, chunk):
        if chunk < 2:
            return wq_hbm.at[index, :, pl.ds(chunk * columns, columns)], wq.at[index, 4 + 2 * chunk]
        return wo_hbm.at[index], wo.at[index, 2]

    def extent(chunk):
        return width if chunk < 2 else depth

    def cut(index, chunk, kind):
        alone, shared = pieces(index, extent(chunk))
        cuts = 2 if chunk < 2 else 1
        size = alone if kind[0] == "a" else shared
        if not size:
            return []
        x_of = x_at if kind[1] == "s" else 1 - x_at
        if kind[0] == "a":
            base = x_of * alone
        else:
            z_of = z_at if kind[2] == "s" else 1 - z_at
            base = 2 * alone + (x_of * 2 + z_of) * shared
        size //= cuts
        return [pl.ds(pl.multiple_of(base + c * size, 16), size) for c in range(cuts)]

    kinds = ("qss", "qso", "qos", "qoo", "as", "ao")
    every = [(index, chunk) for index in range(layers) for chunk in range(3)]
    homes = {which: home(*which) for which in every}
    theres = {
        (index, chunk): wq.at[index, 5 + 2 * chunk] if chunk < 2 else wo.at[index, 3]
        for index, chunk in every
    }
    parts_of = {
        (*which, kind): [homes[which][1].at[at] for at in cut(*which, kind)]
        for which in every
        for kind in kinds
    }

    def first(index, chunk):
        source, _ = homes[index, chunk]
        for kind in ("qss", "as"):
            for c, at in enumerate(cut(index, chunk, kind)):
                part = parts_of[index, chunk, kind][c]
                send(("y", index, chunk, kind, c), source.at[at], part, across)

    def second(index, chunk):
        for c, part in enumerate(parts_of[index, chunk, "qss"]):
            arrive(("y", index, chunk, "qss", c), part)
            send(("x", index, chunk, "q", c), part, part, beside)
            send(("z", index, chunk, "s", c), part, part, above)

    def third(index, chunk):
        for c, part in enumerate(parts_of[index, chunk, "as"]):
            arrive(("y", index, chunk, "as", c), part)
            send(("x", index, chunk, "a", c), part, part, beside)

    def then(index, chunk):
        if index:
            third(index, chunk)
        for c, part in enumerate(parts_of[index, chunk, "qos"]):
            arrive(("x", index, chunk, "q", c), part)
            send(("z", index, chunk, "o", c), part, part, above)

    def fourth(index, chunk):
        for c, part in enumerate(parts_of[index, chunk, "ao"]):
            arrive(("x", index, chunk, "a", c), part)
        for c, part in enumerate(parts_of[index, chunk, "qso"]):
            arrive(("z", index, chunk, "s", c), part)
        for c, part in enumerate(parts_of[index, chunk, "qoo"]):
            arrive(("z", index, chunk, "o", c), part)
        if index or chunk == 2:
            send(("f", index, chunk), homes[index, chunk][1], theres[index, chunk], partner)

    def fifth(index, chunk):
        arrive(("f", index, chunk), theres[index, chunk])

    def share(index, chunk):
        source, _ = home(index, chunk)
        there = wq.at[index, 2 + chunk] if chunk < 2 else wo.at[index, 1]
        send(("w", index, chunk), source, there, partner)

    def shared(index, chunk):
        there = wq.at[index, 2 + chunk] if chunk < 2 else wo.at[index, 1]
        arrive(("w", index, chunk), there)

    def column_of(row):
        return jnp.transpose(jnp.broadcast_to(row.astype(f32), (LANES, row.shape[1])))

    half = rows // 2

    def normed(index, part):
        at = pl.ds(part * half, half)
        xs[index, 0, at, :] = layer_norm(
            stream[at, :].astype(f32), gain_ref[index : index + 1, :]
        )

    def exchange(index, part):
        at = pl.ds(part * half, half)
        send(
            ("n", index, part), xs.at[index, 0, at], xs.at[index, 1, at],
            pair if index else partner,
        )

    def exchanged(index, part):
        arrive(("n", index, part), xs.at[index, 1, pl.ds(part * half, half)])

    pl.semaphore_wait(barrier, 5)
    for chunk in range(3):
        first(0, chunk)
    column = column_of(order_ref[...])[:, :1]
    picks = (column == lax.broadcasted_iota(jnp.int32, (1, rows), 1).astype(f32)).astype(bf16)
    stream[...] = jnp.dot(picks, points_ref[...], preferred_element_type=f32).astype(bf16)
    for part in range(2):
        normed(0, part)
        exchange(0, part)
    spot = (lane % HEAD_DIM).astype(f32)

    def mark(side, row):
        own = column_of(row)
        tag_q[side] = jnp.where((spot < SCANS) & (own != spot), 1.0, 0.0)
        tag_k[side] = jnp.where(own == spot, BLOCKED, 0.0)

    mark(0, tag_ref[...])

    send(("t", 0), tag_ref, tags.at[0], partner)
    send(("t", 1), tag_ref, tags.at[1], pair)
    share(0, 2)
    for chunk in range(3):
        share(1, chunk)
    for chunk in range(3):
        first(1, chunk)

    def place(side, turn, left, right, middle):
        at = pl.ds(side * rows, rows)
        marks = tag_k[side]
        keys[turn, 0, at, :] = jnp.where(low, marks, left).astype(bf16)
        values[turn, 0, at, :] = jnp.where(low, middle, 1.0).astype(bf16)
        keys[turn, 1, at, :] = jnp.where(low, right, marks).astype(bf16)
        values[turn, 1, at, :] = jnp.where(low, 1.0, right).astype(bf16)

    def project(index, k, side, q_at, turn):
        result = jnp.dot(xs[index, side], wq[index, k], preferred_element_type=f32)
        left, middle, right = (result[:, LANES * n : LANES * (n + 1)] for n in range(3))
        place(side, turn, left, right, middle)
        marks = tag_q[side]
        query[q_at, 0] = jnp.where(
            low, marks, pltpu.roll(left * LOG2_SCALE, HEAD_DIM, 1)
        ).astype(bf16)
        query[q_at, 1] = jnp.where(
            low, pltpu.roll(middle * LOG2_SCALE, HEAD_DIM, 1), marks
        ).astype(bf16)

    def project_pair(k, turn):
        left, middle, right = (wq[1, k, :, LANES * n : LANES * (n + 1)] for n in range(3))
        weights = jnp.concatenate([jnp.where(low, middle, left), right], axis=1)
        result = jnp.dot(xs[1, 1], weights, preferred_element_type=f32)
        left, right = result[:, :LANES], result[:, LANES:]
        place(1, turn, left, right, left)

    def scores(q_at, turn, head, at, over):
        return lax.dot_general(
            query[q_at, head, at, :], keys[turn, head, over, :], (((1,), (1,)), ((), ())),
            preferred_element_type=f32,
        )

    def settle(target, k, at, sums):
        parts = [t / pltpu.roll(t, HEAD_DIM, 1) for t in sums]
        target[k, at, :] = jnp.where(low, parts[0], parts[1]).astype(bf16)

    row_blocks = [pl.ds(r * half, half) for r in range(2)]

    def flow(units, beside_first=None):
        table = units[0][0]()
        for n, (_, use) in enumerate(units):
            ahead = units[n + 1][0]() if n + 1 < len(units) else None
            if n == 0 and beside_first is not None:
                beside_first()
            use(table)
            table = ahead

    def attend(side, finish):
        units = []
        for at in row_blocks:
            sums = []
            for head in range(2):
                def look(head=head, at=at):
                    return scores(side, 0, head, at, slice(None))

                def use(table, head=head, at=at, sums=sums):
                    top = jnp.max(table, axis=-1, keepdims=True)
                    expo = jnp.exp2(table - top).astype(bf16)
                    sums.append(
                        jnp.dot(expo, values[0, head], preferred_element_type=f32)
                    )
                    if head == 1:
                        finish(at, sums)

                units.append((look, use))
        return units

    def attend_own(k, turn):
        over = pl.ds(0, rows)
        units = []
        for at in row_blocks:
            for head in range(2):
                def look(head=head, at=at):
                    return scores(k, turn, head, at, over)

                def use(table, head=head, at=at):
                    top = jnp.max(table, axis=-1, keepdims=True)
                    expo = jnp.exp2(table - top).astype(bf16)
                    acc[k, head, at, :] = jnp.dot(
                        expo, values[turn, head, over, :], preferred_element_type=f32
                    )
                    peak[k, head, at, :] = jnp.broadcast_to(top, (half, LANES))

                units.append((look, use))
        return units

    def attend_pair(k, turn):
        over = pl.ds(rows, rows)
        units = []
        for at in row_blocks:
            sums = []
            for head in range(2):
                def look(head=head, at=at):
                    return scores(k, turn, head, at, over)

                def use(table, head=head, at=at, sums=sums):
                    before = peak[k, head, at, :]
                    highest = jnp.max(table, axis=-1, keepdims=True)
                    top = jnp.maximum(before, jnp.broadcast_to(highest, (half, LANES)))
                    expo = jnp.concatenate(
                        [
                            jnp.exp2(table[:, LANES * n : LANES * (n + 1)] - top).astype(bf16)
                            for n in range(rows // LANES)
                        ],
                        axis=1,
                    )
                    sums.append(
                        jnp.dot(expo, values[turn, head, over, :], preferred_element_type=f32)
                        + acc[k, head, at, :] * jnp.exp2(before - top)
                    )
                    if head == 1:
                        settle(att, k, at, sums)

                units.append((look, use))
        return units

    def leave(index, part):
        at = pl.ds(part * half, half)
        result = stream[at, :].astype(f32)
        for slot, (one, two) in enumerate(((0, 1), (2, 3), (4, 6), (5, 7))):
            result += jnp.dot(
                jnp.concatenate([att[one, at, :], att[two, at, :]], axis=1),
                wo[index, slot],
                preferred_element_type=f32,
            )
        return result.astype(bf16)

    def run(count, events, *phases):
        def step(k, carry):
            for n, phase in enumerate(phases):
                for (when, place_in), todo in events.items():
                    if place_in == n:

                        @pl.when(k == when)
                        def _(todo=todo):
                            for event, args in todo:
                                event(*args)

                phase(k)
            return carry

        lax.fori_loop(0, count, step, 0)

    arrive(("t", 0), tags.at[0])
    mark(1, tags[0])
    exchanged(0, 0)
    exchanged(0, 1)

    def loaded(n):
        load(n).wait()

    def slot_of(k):
        return k + k // 2 * k

    def handed(k):
        to = 2 + k + k // 2 * (k - 1)
        return remote(given.at[k], att.at[to], given_send.at[k], given_recv.at[k], partner)

    def taken(k):
        to = 2 + k + k // 2 * (k - 1)
        part = att.at[to]
        return remote(part, part, given_send.at[k], given_recv.at[k], partner)

    def make(k):
        slot = slot_of(k)
        for side in range(2):
            project(0, slot, side, side, 0)

    def weigh(k):
        def give(at, sums):
            settle(given, k, at, sums)
            if at is row_blocks[-1]:
                handed(k).start()

        def keep(at, sums):
            settle(att, slot_of(k), at, sums)

        flow(attend(1, give) + attend(0, keep))

    run(
        4,
        {
            (0, 0): [(loaded, (0,)), (loaded, (1,))],
            (0, 1): [(second, (0, 0))],
            (1, 0): [(third, (0, 0)), (then, (0, 0))],
            (1, 1): [(second, (0, 1)), (third, (0, 1))],
            (2, 0): [(then, (0, 1)), (fourth, (0, 0))],
            (2, 1): [(second, (0, 2)), (third, (0, 2))],
            (3, 0): [(then, (0, 2)), (fourth, (0, 1)), (second, (1, 0))],
            (3, 1): [(fourth, (0, 2))],
        },
        make, weigh,
    )
    then(1, 0)
    second(1, 1)
    loaded(2)
    shared(0, 2)
    fifth(0, 2)
    for k in range(4):
        taken(k).wait_recv()
    for part in range(2):
        at = pl.ds(part * half, half)
        stream[at, :] = leave(0, part)
        normed(1, part)
        exchange(1, part)
    then(1, 1)
    second(1, 2)
    arrive(("t", 1), tags.at[1])
    mark(1, tags[1])

    loaded(3)
    loaded(4)
    project(1, 0, 0, 0, 0)

    def inner(k):
        flow(attend_own(k, k % 2), lambda: project(1, k + 1, 0, k + 1, (k + 1) % 2))

    run(
        steps - 1,
        {
            (1, 0): [(shared, (1, 0)), (fourth, (1, 0))],
            (2, 0): [(shared, (1, 1))],
            (3, 0): [],
            (4, 0): [(fifth, (1, 0)), (fourth, (1, 1))],
            (6, 0): [(then, (1, 2)), (fifth, (1, 1))],
        },
        inner,
    )
    flow(attend_own(steps - 1, 1))
    exchanged(1, 0)
    exchanged(1, 1)
    fourth(1, 2)

    project_pair(0, 0)

    def outer(k):
        flow(attend_pair(k, k % 2), lambda: project_pair(k + 1, (k + 1) % 2))

    run(steps - 1, {}, outer)
    flow(attend_pair(steps - 1, 1))
    loaded(5)
    shared(1, 2)
    fifth(1, 2)
    for part in range(2):
        out_ref[pl.ds(part * half, half), :] = leave(1, part)

    for key, src, dst, device in order_of_sends:
        copy(key, src, dst, device).wait_send()
    for k in range(4):
        handed(k).wait_send()


def fused(points, order, scan_ids, ln_gain, w_qkv, w_out):
    rows, width = points.shape
    peers, ranges = lax.axis_size("head"), lax.axis_size("curve")
    layers, _, columns = w_qkv.shape
    columns //= 2
    steps = 2 * peers
    vmem, far = pl.BlockSpec(memory_space=pltpu.VMEM), pl.BlockSpec(memory_space=pl.ANY)
    dma = pltpu.SemaphoreType.DMA
    bf16, f32 = jnp.bfloat16, jnp.float32
    return pl.pallas_call(
        functools.partial(fused_kernel, peers, ranges),
        out_shape=jax.ShapeDtypeStruct((rows, width), bf16),
        in_specs=[vmem] * 4 + [far] * 2,
        out_specs=vmem,
        scratch_shapes=[
            pltpu.VMEM((layers, 2, rows, width), bf16),
            pltpu.VMEM((rows, width), bf16),
            pltpu.VMEM((layers, steps, width, columns), bf16),
            pltpu.VMEM((layers, peers, width // peers, width), bf16),
            pltpu.VMEM((steps, 2, rows, LANES), bf16),
            pltpu.VMEM((2, 2, 2 * rows, LANES), bf16),
            pltpu.VMEM((2, 2, 2 * rows, LANES), bf16),
            pltpu.VMEM((steps, rows, LANES), bf16),
            pltpu.VMEM((steps, 2, rows, LANES), f32),
            pltpu.VMEM((steps, 2, rows, LANES), f32),
            pltpu.VMEM((2, 1, rows), jnp.int32),
            pltpu.VMEM((2, rows, LANES), f32),
            pltpu.VMEM((2, rows, LANES), f32),
            pltpu.VMEM((steps // 2, rows, LANES), bf16),
            dma((96,)),
            dma((96,)),
            dma((3 * layers,)),
            dma((steps // 2,)),
            dma((steps // 2,)),
        ],
        compiler_params=pltpu.CompilerParams(
            collective_id=0, has_side_effects=True, vmem_limit_bytes=60 * 1024 * 1024
        ),
        cost_estimate=pl.CostEstimate(
            flops=80 * rows * width * width, bytes_accessed=20 * rows * width, transcendentals=0
        ),
    )(points, order, scan_ids.reshape(1, -1), ln_gain, w_qkv, w_out)


def chip_holds_window(points, w_qkv):
    peers, ranges = lax.axis_size("head"), lax.axis_size("curve")
    rows, width = points.shape
    return (
        peers == 4
        and ranges % 4 == 0
        and PATCH == 2 * rows
        and w_qkv.shape[0] == 2
        and w_qkv.shape[2] == 12 * HEAD_DIM
        and width == peers * 4 * HEAD_DIM
    )


def on_device(points, order, scan_ids, ln_gain, w_qkv, w_out):
    if chip_holds_window(points, w_qkv):
        return fused(points, order, scan_ids, ln_gain, w_qkv, w_out)
    stream = points[order[0]]
    tag_row = scan_ids.reshape(1, 1, -1)
    for index in range(2):
        normed = layer_norm(stream, ln_gain[index])
        stream = layer(index, stream, normed, tag_row, w_qkv[index], w_out[index])
    return stream


def solution(mesh):
    in_specs = (
        P(("curve", "head"), None),
        P(("curve", "head"), None),
        P(("curve", "head")),
        P(),
        P(None, None, "head"),
        P(None, "head", None),
    )
    out_specs = P(("curve", "head"), None)
    return jax.shard_map(
        on_device, mesh=mesh, in_specs=in_specs, out_specs=out_specs, check_vma=False
    )
```
